32 devices in a mesh: group: 2 (over y), tm: 4 (over z), bl: 2 (over x), pol: 2 (over core).
Axes of the slice: x: 2, y: 2, z: 4, core: 2. Of those that a mesh axis runs over, the one named last changes fastest.
Arguments:
- visibilities: bfloat16 [1600, 256, 2, 384], P(('group', 'tm'), ('bl', 'pol')), parts along dimension 0, may hold values from -6 to 6
- flag_mask: int32 [1600], P(('group', 'tm')), parts along dimension 0, may hold values 0 or 1
- kernel_index: int32 [256], P(('bl', 'pol')), may hold values from 0 to 15
- filter_bank: float32 [2, 16, 257], replicated, may hold values from -0.875 to 0.875
Outputs:
- fringe_filtered: bfloat16 [160, 256, 2, 384], P('group', ('bl', 'pol', 'tm')), parts along dimension 0
The draws below stay inside these ranges and needn't reach their ends.
There are 2 independent parts, one for each index of `group`. The reference program is written for one: setup_inputs(seed, part) draws one part's arguments, and reference() takes and returns one part's arrays. A program takes and returns all parts, laid end to end along the dimension named above; an argument that names none is the same for every part. Nothing has to cross between parts.
All inputs are finite; a program needn't handle non-finite values. No bound on the sum of `flag_mask` on one device may be relied on, other than what follows from the above.
Results may differ from the reference program's by a relative error of at most 0.001.
Values may be sent and summed in bfloat16 or wider, within the bound.
A program may use at most 192 MiB of HBM per device.

```python
import jax
import jax.numpy as jnp
from jax import lax

BASE = 256
CHAN = 384
TAPS = 257
AVG = 10
NKERN = 16
T_DEV = 200
TIMES = 800
OUT_TIMES = 80


def place_ends(array, stream_key, least, top_value):
    index_at = [jax.random.randint(jax.random.fold_in(stream_key, axis), (), 0, length) for axis, length in enumerate(array.shape)]
    widest = array.shape.index(max(array.shape))
    neighbour = index_at[:widest] + [(index_at[widest] + 1) % array.shape[widest]] + index_at[widest + 1:]
    return array.at[tuple(index_at)].set(least).at[tuple(neighbour)].set(top_value)


def block_levels(own_key, shape, shards, smallest, largest):
    level, own = 1.0, jax.random.fold_in(own_key, 6)
    for position, shards_of in shards:
        draws = jnp.exp(jax.random.uniform(jax.random.fold_in(own, position), (shards_of,), jnp.float32, smallest / len(shards), largest / len(shards)))
        level = level * jnp.repeat(draws, shape[position] // shards_of).reshape([-1 if axis == position else 1 for axis in range(len(shape))])
    return level


def gaussian(own_key, shape, scale, limit, pieces=(), kind=jnp.bfloat16):
    factor_of = block_levels(own_key, shape, pieces, -0.22, 0.18) if pieces else 1.0
    entries = jax.random.normal(own_key, shape, jnp.float32) * scale * factor_of
    return jnp.minimum(jnp.maximum(entries, -limit), limit).astype(kind)


def setup_inputs(seed: int = 0, part: int = 0) -> dict:
    keys = jax.random.split(jax.random.key(seed), 5)
    part_splits = jax.random.split(jax.random.fold_in(keys[4], part), 5)
    visibilities = gaussian(part_splits[0], (TIMES, BASE, 2, CHAN), 1.0, 6.0, ((0, 4), (1, 4)))
    flag_mask = place_ends((jax.random.randint(part_splits[1], (TIMES,), 0, 10) < 9).astype(jnp.int32), jax.random.fold_in(part_splits[1], 1), 0, 1)
    kernel_index = place_ends(jax.random.randint(keys[2], (BASE,), 0, NKERN), jax.random.fold_in(keys[2], 1), 0, NKERN - 1).astype(jnp.int32)
    filter_bank = gaussian(keys[3], (2, NKERN, TAPS), (TAPS // 5) ** -0.5, 0.875, (), jnp.float32)
    return {"visibilities": visibilities, "flag_mask": flag_mask, "kernel_index": kernel_index, "filter_bank": filter_bank}


def select_taps(kernel_index, filter_bank):
    choices_count = filter_bank.shape[1]
    one_hot = (kernel_index[:, None] == jnp.arange(choices_count, dtype=jnp.int32)[None, :]).astype(jnp.float32)
    return jnp.einsum("bk,rkt->brt", one_hot, filter_bank, precision=lax.Precision.HIGHEST)


def make_band(kernel_taps, block_rows):
    tap_count = kernel_taps.shape[1]
    row_width = block_rows + tap_count - 1
    zero_tail = jnp.zeros((2, block_rows), jnp.float32)
    period_row = jnp.concatenate([kernel_taps, zero_tail], axis=1)
    tiled_rows = jnp.tile(period_row, (1, block_rows))[:, :block_rows * row_width]
    return tiled_rows.reshape(2, block_rows, row_width)


def filter_block(time_slab, kernel_taps, block_rows, joined_average):
    band_rows = make_band(kernel_taps, block_rows)
    row_width = band_rows.shape[2]
    if joined_average:
        band_rows = band_rows.reshape(2, block_rows // AVG, AVG, row_width).sum(axis=2) * (1.0 / AVG)
    out_count = band_rows.shape[1]
    stacked = band_rows.reshape(2 * out_count, row_width)
    product = jnp.dot(stacked, time_slab, precision=lax.Precision.HIGHEST, preferred_element_type=jnp.float32)
    prod_real = product[:out_count]
    prod_imag = product[out_count:]
    channels = time_slab.shape[1] // 2
    out_real = prod_real[:, :channels] - prod_imag[:, channels:]
    out_imag = prod_real[:, channels:] + prod_imag[:, :channels]
    result = jnp.stack([out_real, out_imag], axis=1)
    if not joined_average:
        result = result.reshape(out_count // AVG, AVG, 2, channels).sum(axis=1) * (1.0 / AVG)
    return result


def reference(visibilities, flag_mask, kernel_index, filter_bank):
    half_taps = TAPS // 2
    flag_float = flag_mask.astype(jnp.float32)
    taps_all = select_taps(kernel_index, filter_bank)
    block_count = TIMES // T_DEV

    def per_base(base_index):
        column = lax.dynamic_index_in_dim(visibilities, base_index, 1, False).astype(jnp.float32)
        column = (column * flag_float[:, None, None]).reshape(TIMES, 2 * CHAN)
        padded = jnp.pad(column, ((half_taps, half_taps), (0, 0)))
        kernel_taps = lax.dynamic_index_in_dim(taps_all, base_index, 0, False)

        def per_block(block_index):
            time_slab = lax.dynamic_slice_in_dim(padded, (block_index * T_DEV).astype(jnp.int32), T_DEV + TAPS - 1, 0)
            return filter_block(time_slab, kernel_taps, T_DEV, True)

        blocks_out = lax.map(per_block, jnp.arange(block_count, dtype=jnp.int32))
        return blocks_out.reshape(OUT_TIMES, 2, CHAN)

    filtered = lax.map(per_base, jnp.arange(BASE, dtype=jnp.int32))
    return jnp.moveaxis(filtered, 0, 1).astype(jnp.bfloat16)
```

```python
import functools

import jax
import jax.numpy as jnp
from jax import lax
from jax.experimental import pallas as pl
from jax.experimental.pallas import tpu as pltpu
from jax.sharding import PartitionSpec as P

TAPS = 257
AVG = 10
HALF = TAPS // 2
SIDE = -(-HALF // AVG)
GROUP = 8
LOADS = 3
LEVELS = 32767.0
TINY = 1e-33


def round_up(value, step):
    return -(-value // step) * step


def row_plan(block_rows):
    out_count = block_rows // AVG
    edge, mid = out_count, 2 * SIDE - out_count
    assert 0 < mid < SIDE <= out_count
    edge_rows, mid_rows = round_up(2 * edge, 8), round_up(2 * mid, 8)
    total_rows = 2 * edge_rows + mid_rows
    highest = 2 * (block_rows + HALF + AVG * SIDE)
    lowest = 2 * HALF - 2 * AVG * (SIDE + edge)
    period = round_up(max(highest, 2 * (TAPS + AVG) - lowest), 128)
    return out_count, edge, mid, edge_rows, mid_rows, total_rows, period


def averaged_taps(filter_bank, period):
    width = TAPS + AVG - 1
    padded = jnp.pad(filter_bank, ((0, 0), (0, 0), (AVG - 1, AVG - 1)))
    total = padded[:, :, 0:width]
    for shift in range(1, AVG):
        total = total + padded[:, :, shift : shift + width]
    real, imag = total[0] * (1.0 / AVG), total[1] * (1.0 / AVG)
    to_real = jnp.stack([real, -imag], axis=-1).reshape(-1, 2 * width)
    to_imag = jnp.stack([imag, real], axis=-1).reshape(-1, 2 * width)
    to_real = jnp.pad(to_real, ((0, 0), (0, period - 2 * width)))
    to_imag = jnp.pad(to_imag, ((0, 0), (0, period - 2 * width)))
    return jnp.stack([to_real, jnp.roll(to_imag, -AVG, axis=1)], axis=1)


def build_bands(taps_ref, flag_ref, band_ref, block_rows):
    out_count, edge, mid, edge_rows, mid_rows, total_rows, period = row_plan(block_rows)
    flags = flag_ref[...].astype(jnp.float32)
    runs = ((-SIDE, edge, edge_rows), (out_count - SIDE, mid, mid_rows), (SIDE, edge, edge_rows))

    def one_filter(f, carry):
        base = jnp.concatenate([taps_ref[f]] * 4, axis=0)
        tile = pltpu.roll(base, 0, 1, stride=AVG, stride_axis=0)
        tiles = []
        for first, count, rows in runs:
            for row in range(0, rows, 8):
                shift = (2 * AVG * first + AVG * row - 2 * HALF) % period
                piece = pltpu.roll(tile, shift, 1)[:, : 2 * block_rows] * flags
                if row + 8 > 2 * count:
                    at = lax.broadcasted_iota(jnp.int32, piece.shape, 0)
                    piece = jnp.where(at < 2 * count - row, piece, 0.0)
                tiles.append(piece)
        band = jnp.concatenate(tiles, axis=0)
        high = band.astype(jnp.bfloat16)
        band_ref[f, :total_rows, :] = high
        band_ref[f, total_rows:, :] = (band - high.astype(jnp.float32)).astype(jnp.bfloat16)
        return carry

    lax.fori_loop(0, taps_ref.shape[0], one_filter, 0, unroll=4)


def band_kernel(taps_ref, flag_ref, band_ref, *, block_rows):
    build_bands(taps_ref, flag_ref, band_ref, block_rows)


def band_call(taps, flags):
    block_rows = flags.shape[1] // 2
    total_rows = row_plan(block_rows)[5]
    return pl.pallas_call(
        functools.partial(band_kernel, block_rows=block_rows),
        in_specs=[pl.BlockSpec(memory_space=pltpu.VMEM)] * 2,
        out_specs=pl.BlockSpec(memory_space=pltpu.VMEM),
        out_shape=jax.ShapeDtypeStruct(
            (taps.shape[0], 2 * total_rows, 2 * block_rows), jnp.bfloat16
        ),
    )(taps, flags)


def encode(value, code_ref, step_ref, i):
    peak = jnp.max(jnp.max(jnp.abs(value), axis=0, keepdims=True), axis=1, keepdims=True)
    peak = jnp.maximum(peak, TINY)
    step_ref[i : i + 1, :] = jnp.broadcast_to(peak * (1.0 / LEVELS), (1, step_ref.shape[1]))
    code = jnp.round(value * (LEVELS / peak)).astype(jnp.int32).astype(jnp.int16)
    code_ref[:, i] = code.reshape(-1, 2, value.shape[1])


def decode(code):
    rows = code.astype(jnp.int32).astype(jnp.float32)
    return rows.reshape(2 * code.shape[0], code.shape[2])


def stream_kernel(
    index_ref,
    band_ref,
    vis_ref,
    out_ref,
    slab_ref,
    sum_ref,
    edge_ref,
    edge_step_ref,
    mid_ref,
    mid_step_ref,
    in_ref,
    in_edge_step_ref,
    in_mid_step_ref,
    done_ref,
    own_ref,
    load_sem,
    edge_send,
    edge_step_send,
    mid_send,
    mid_step_send,
    edge_recv,
    edge_step_recv,
    mid_recv,
    mid_step_recv,
    done_send,
    done_recv,
    own_sem,
    *,
    count,
):
    me = lax.axis_index("tm")
    _, block_rows, group, _, channels = slab_ref.shape
    chunks = done_ref.shape[0]
    per_owner = chunks // count
    out_count, edge, mid, edge_rows, mid_rows, total_rows, _ = row_plan(block_rows)
    alone = out_count - SIDE
    mid_at, far_at = edge_rows, edge_rows + mid_rows
    has_left, has_right = me > 0, me < count - 1
    nearer, farther = jnp.minimum(me, count - 1 - me), jnp.maximum(me, count - 1 - me)
    sign = jnp.where(2 * me <= count - 1, 1, -1)

    def chunk_at(step):
        turn, part = step // per_owner, step % per_owner
        late = turn - (farther - nearer)
        flip = jnp.where(late % 2 == 0, sign, -sign)
        owner = jnp.where(
            late < 0, me + sign * (farther - turn), me + flip * (nearer - late // 2)
        )
        return owner, part, owner * per_owner + part

    def load(step):
        _, _, chunk = chunk_at(step)
        slot = step % LOADS
        return pltpu.make_async_copy(
            vis_ref.at[:, pl.ds(chunk * group, group)], slab_ref.at[slot], load_sem.at[slot]
        )

    def remote(source, target, send_sem, recv_sem, device):
        return pltpu.make_async_remote_copy(
            src_ref=source,
            dst_ref=target,
            send_sem=send_sem,
            recv_sem=recv_sem,
            device_id={"tm": device},
            device_id_type=pl.DeviceIdType.MESH,
        )

    def slot_of(owner, part, chunk, receiver, rightward):
        second = jnp.logical_and(owner == receiver, jnp.logical_not(rightward))
        return jnp.where(second, chunks + part, chunk)

    def edge_copies(chunk, slot, rightward, device):
        start = jnp.where(rightward, mid, 0)
        return (
            remote(
                edge_ref.at[chunk],
                in_ref.at[slot, pl.ds(start, edge)],
                edge_send.at[chunk],
                edge_recv.at[slot],
                device,
            ),
            remote(
                edge_step_ref.at[chunk],
                in_edge_step_ref.at[slot],
                edge_step_send.at[chunk],
                edge_step_recv.at[slot],
                device,
            ),
        )

    def mid_copies(chunk, slot, rightward, device):
        start = jnp.where(rightward, 0, edge)
        return (
            remote(
                mid_ref.at[chunk],
                in_ref.at[slot, pl.ds(start, mid)],
                mid_send.at[chunk],
                mid_recv.at[slot],
                device,
            ),
            remote(
                mid_step_ref.at[chunk],
                in_mid_step_ref.at[slot],
                mid_step_send.at[chunk],
                mid_step_recv.at[slot],
                device,
            ),
        )

    def placed(row, rows, part):
        return out_ref.at[pl.ds(row, rows), pl.ds(part * group, group)]

    def full_done(source, chunk, part, rightward, device):
        row = jnp.where(rightward, out_count * (source - 1) + alone, out_count * source + SIDE)
        return remote(
            done_ref.at[chunk],
            placed(row, edge, part),
            done_send.at[chunk],
            done_recv.at[source, part],
            device,
        )

    def short_done(source, chunk, part, rightward, device):
        row = jnp.where(rightward, 0, out_count * source + SIDE)
        start = jnp.where(rightward, SIDE, 0)
        return remote(
            done_ref.at[chunk, pl.ds(start, alone)],
            placed(row, alone, part),
            done_send.at[chunk],
            done_recv.at[source, part],
            device,
        )

    def keep(part, low, rows):
        return pltpu.make_async_copy(
            own_ref.at[part, pl.ds(low, rows)],
            placed(jnp.maximum(out_count * me - SIDE, 0), rows, part),
            own_sem.at[part],
        )

    for step in range(LOADS - 1):
        load(step).start()
    barrier = pltpu.get_barrier_semaphore()
    for offset in range(1, count):
        pl.semaphore_signal(
            barrier,
            inc=1,
            device_id={"tm": lax.rem(me + offset, count)},
            device_id_type=pl.DeviceIdType.MESH,
        )
    pl.semaphore_wait(barrier, count - 1)

    def flow(owner):
        rightward = owner > me
        upstream = jnp.where(rightward, has_left, has_right)
        return rightward, upstream, jnp.where(rightward, me + 1, me - 1)

    def compute(step, carry):
        @pl.when(step + LOADS - 1 < chunks)
        def _():
            load(step + LOADS - 1).start()

        load(step).wait()
        owner, part, chunk = chunk_at(step)
        slot = step % LOADS
        rightward, upstream, target = flow(owner)
        landing = slot_of(owner, part, chunk, target, rightward)
        for i in range(group):
            which = index_ref[chunk * group + i]
            slab = slab_ref[slot, :, i].reshape(2 * block_rows, channels)
            both = jnp.dot(band_ref[which], slab, preferred_element_type=jnp.float32)
            sum_ref[chunk, i] = both[:total_rows] + both[total_rows:]

        @pl.when(owner != me)
        def _():
            start = pl.multiple_of(jnp.where(rightward, far_at, 0), 8)
            for i in range(group):
                encode(
                    sum_ref[chunk, i, pl.ds(start, 2 * edge), :],
                    edge_ref.at[chunk],
                    edge_step_ref.at[chunk],
                    i,
                )
            for copy in edge_copies(chunk, landing, rightward, target):
                copy.start()

        @pl.when(jnp.logical_and(owner != me, jnp.logical_not(upstream)))
        def _():
            for i in range(group):
                encode(
                    sum_ref[chunk, i, mid_at : mid_at + 2 * mid, :],
                    mid_ref.at[chunk],
                    mid_step_ref.at[chunk],
                    i,
                )
            for copy in mid_copies(chunk, landing, rightward, target):
                copy.start()

        return carry

    lax.fori_loop(0, chunks, compute, 0)

    def step_of(step_ref, slot, i):
        return jnp.concatenate([step_ref[slot, i : i + 1, :]] * (channels // 128), axis=1)

    def finish(step, carry):
        owner, part, chunk = chunk_at(step)
        rightward, upstream, target = flow(owner)
        landing = slot_of(owner, part, chunk, target, rightward)
        forward = owner != me

        @pl.when(jnp.logical_and(forward, upstream))
        def _():
            for copy in edge_copies(chunk, chunk, rightward, target):
                copy.wait_recv()
            start = jnp.where(rightward, edge, 0)
            for i in range(group):
                came = decode(in_ref[chunk, pl.ds(start, mid), i])
                value = sum_ref[chunk, i, mid_at : mid_at + 2 * mid, :]
                value = value + came * step_of(in_edge_step_ref, chunk, i)
                encode(value, mid_ref.at[chunk], mid_step_ref.at[chunk], i)
            for copy in mid_copies(chunk, landing, rightward, target):
                copy.start()
            for copy in mid_copies(chunk, chunk, rightward, target):
                copy.wait_recv()
            start = jnp.where(rightward, 0, mid)
            near = pl.multiple_of(jnp.where(rightward, 0, far_at), 8)
            at = lax.broadcasted_iota(jnp.int32, (2 * edge, channels), 0)
            first = jnp.where(rightward, 0, 2 * (edge - mid))
            of_mid = jnp.logical_and(at >= first, at < first + 2 * mid)
            for i in range(group):
                came = decode(in_ref[chunk, pl.ds(start, edge), i])
                unit = jnp.where(
                    of_mid,
                    step_of(in_mid_step_ref, chunk, i),
                    step_of(in_edge_step_ref, chunk, i),
                )
                value = sum_ref[chunk, i, pl.ds(near, 2 * edge), :] + came * unit
                done_ref[chunk, :, i] = value.astype(jnp.bfloat16).reshape(edge, 2, channels)
            full_done(me, chunk, part, rightward, owner).start()

        @pl.when(jnp.logical_and(forward, jnp.logical_not(upstream)))
        def _():
            near = pl.multiple_of(jnp.where(rightward, 0, far_at), 8)
            for i in range(group):
                value = sum_ref[chunk, i, pl.ds(near, 2 * edge), :]
                done_ref[chunk, :, i] = value.astype(jnp.bfloat16).reshape(edge, 2, channels)
            short_done(me, chunk, part, rightward, owner).start()

        def from_side(slot, rightward, near, edge_start, first):
            for copy in edge_copies(chunk, slot, rightward, me):
                copy.wait_recv()
            for copy in mid_copies(chunk, slot, rightward, me):
                copy.wait_recv()
            at = lax.broadcasted_iota(jnp.int32, (2 * edge, channels), 0)
            of_mid = jnp.logical_and(at >= first, at < first + 2 * mid)
            for i in range(group):
                edge_unit = step_of(in_edge_step_ref, slot, i)
                unit = jnp.where(of_mid, step_of(in_mid_step_ref, slot, i), edge_unit)
                came = decode(in_ref[slot, edge_start : edge_start + edge, i])
                sum_ref[chunk, i, near : near + 2 * edge, :] += came * unit
                start = edge if rightward else 0
                came = decode(in_ref[slot, start : start + mid, i])
                sum_ref[chunk, i, mid_at : mid_at + 2 * mid, :] += came * edge_unit

        @pl.when(jnp.logical_and(owner == me, has_left))
        def _():
            from_side(chunk, True, 0, 0, 0)

        @pl.when(jnp.logical_and(owner == me, has_right))
        def _():
            from_side(chunks + part, False, far_at, mid, 2 * (edge - mid))

        @pl.when(owner == me)
        def _():
            for i in range(group):
                for row, rows, start in (
                    (0, edge, 0),
                    (edge, mid, mid_at),
                    (edge + mid, edge, far_at),
                ):
                    value = sum_ref[chunk, i, start : start + 2 * rows, :].astype(jnp.bfloat16)
                    own_ref[part, row : row + rows, i] = value.reshape(rows, 2, channels)

            @pl.when(jnp.logical_and(has_left, has_right))
            def _():
                keep(part, 0, 2 * edge + mid).start()

            @pl.when(jnp.logical_not(has_left))
            def _():
                keep(part, SIDE, out_count + SIDE).start()

            @pl.when(jnp.logical_not(has_right))
            def _():
                keep(part, 0, out_count + SIDE).start()

        return carry

    lax.fori_loop(0, chunks, finish, 0)

    def drain(step, carry):
        owner, part, chunk = chunk_at(step)
        rightward, upstream, target = flow(owner)

        @pl.when(owner != me)
        def _():
            for copy in edge_copies(chunk, chunk, rightward, target):
                copy.wait_send()
            for copy in mid_copies(chunk, chunk, rightward, target):
                copy.wait_send()

            @pl.when(upstream)
            def _():
                full_done(me, chunk, part, rightward, owner).wait_send()

            @pl.when(jnp.logical_not(upstream))
            def _():
                short_done(me, chunk, part, rightward, owner).wait_send()

        @pl.when(owner == me)
        def _():
            @pl.when(jnp.logical_and(has_left, has_right))
            def _():
                keep(part, 0, 2 * edge + mid).wait()

            @pl.when(jnp.logical_not(jnp.logical_and(has_left, has_right)))
            def _():
                keep(part, 0, out_count + SIDE).wait()

        return carry

    lax.fori_loop(0, chunks, drain, 0)

    def collect(turn, carry):
        source = lax.rem(me + 1 + turn, count)
        end = jnp.logical_or(source == 0, source == count - 1)
        for part in range(per_owner):

            @pl.when(end)
            def _():
                short_done(source, 0, part, source < me, source).wait_recv()

            @pl.when(jnp.logical_not(end))
            def _():
                full_done(source, 0, part, source < me, source).wait_recv()

        return carry

    lax.fori_loop(0, count - 1, collect, 0)


def stream_call(kernel_index, bands, visibilities):
    block_rows, bases, _, channels = visibilities.shape
    count = lax.axis_size("tm")
    out_count, edge, mid, _, _, total_rows, _ = row_plan(block_rows)
    owned = bases // count
    group = GROUP
    while owned % group:
        group //= 2
    chunks, parts = bases // group, owned // group
    slots = chunks + parts
    sent, landed = pltpu.SemaphoreType.DMA((chunks,)), pltpu.SemaphoreType.DMA((slots,))
    return pl.pallas_call(
        functools.partial(stream_kernel, count=count),
        in_specs=[
            pl.BlockSpec(memory_space=pltpu.SMEM),
            pl.BlockSpec(memory_space=pltpu.VMEM),
            pl.BlockSpec(memory_space=pl.ANY),
        ],
        out_specs=pl.BlockSpec(memory_space=pl.ANY),
        out_shape=jax.ShapeDtypeStruct((count * out_count, owned, 2, channels), jnp.bfloat16),
        scratch_shapes=[
            pltpu.VMEM((LOADS, block_rows, group, 2, channels), jnp.bfloat16),
            pltpu.VMEM((chunks, group, total_rows, channels), jnp.float32),
            pltpu.VMEM((chunks, edge, group, 2, channels), jnp.int16),
            pltpu.VMEM((chunks, group, 128), jnp.float32),
            pltpu.VMEM((chunks, mid, group, 2, channels), jnp.int16),
            pltpu.VMEM((chunks, group, 128), jnp.float32),
            pltpu.VMEM((slots, edge + mid, group, 2, channels), jnp.int16),
            pltpu.VMEM((slots, group, 128), jnp.float32),
            pltpu.VMEM((slots, group, 128), jnp.float32),
            pltpu.VMEM((chunks, edge, group, 2, channels), jnp.bfloat16),
            pltpu.VMEM((parts, 2 * edge + mid, group, 2, channels), jnp.bfloat16),
            pltpu.SemaphoreType.DMA((LOADS,)),
            sent,
            sent,
            sent,
            sent,
            landed,
            landed,
            landed,
            landed,
            sent,
            pltpu.SemaphoreType.DMA((count, parts)),
            pltpu.SemaphoreType.DMA((parts,)),
        ],
        compiler_params=pltpu.CompilerParams(
            collective_id=0, has_side_effects=True, vmem_limit_bytes=56 * 1024 * 1024
        ),
    )(kernel_index, bands, visibilities)


def per_device(visibilities, flag_mask, kernel_index, filter_bank):
    period = row_plan(visibilities.shape[0])[6]
    taps = averaged_taps(filter_bank, period)
    flags = jnp.repeat(flag_mask, 2)[None, :]
    bands = band_call(taps, flags)
    return stream_call(kernel_index, bands, visibilities)


def solution(mesh):
    placed = (
        P(("group", "tm"), ("bl", "pol"), None, None),
        P(("group", "tm")),
        P(("bl", "pol")),
        P(),
    )
    return jax.shard_map(
        per_device,
        mesh=mesh,
        in_specs=placed,
        out_specs=P("group", ("bl", "pol", "tm"), None, None),
        check_vma=False,
    )
```

```python
import functools

import jax
import jax.numpy as jnp
from jax import lax
from jax.experimental import pallas as pl
from jax.experimental.pallas import tpu as pltpu
from jax.sharding import PartitionSpec as P

TAPS = 257
AVG = 10
HALF = TAPS // 2
SIDE = -(-HALF // AVG)
GROUP = 8
LOADS = 3
LEVELS = 32767.0
TINY = 1e-33


def round_up(value, step):
    return -(-value // step) * step


def row_plan(block_rows):
    out_count = block_rows // AVG
    edge, mid = out_count, 2 * SIDE - out_count
    assert 0 < mid < SIDE <= out_count
    edge_rows, mid_rows = round_up(2 * edge, 8), round_up(2 * mid, 8)
    total_rows = 2 * edge_rows + mid_rows
    highest = 2 * (block_rows + HALF + AVG * SIDE)
    lowest = 2 * HALF - 2 * AVG * (SIDE + edge)
    period = round_up(max(highest, 2 * (TAPS + AVG) - lowest), 128)
    return out_count, edge, mid, edge_rows, mid_rows, total_rows, period


def spread_taps(bank_ref):
    filters, taps = bank_ref.shape[1:]
    width = round_up(2 * (taps + AVG), 128)
    parts = []
    for part in (bank_ref[0], bank_ref[1]):
        for _ in range(3):
            parts.append(part.astype(jnp.bfloat16))
            part = part - parts[-1].astype(jnp.float32)
    ahead = lax.broadcasted_iota(jnp.int32, (taps, width), 1)
    ahead = ahead - 2 * lax.broadcasted_iota(jnp.int32, (taps, width), 0)
    hit = jnp.logical_and(jnp.logical_and(ahead >= 0, ahead < 2 * AVG), ahead % 2 == 0)
    spread = jnp.where(hit, 1.0, 0.0).astype(jnp.bfloat16)
    total = jnp.dot(jnp.concatenate(parts, axis=0), spread, preferred_element_type=jnp.float32)
    total = [total[filters * k : filters * (k + 1)] for k in range(6)]
    real = (total[0] + total[1] + total[2]) * (1.0 / AVG)
    imag = (total[3] + total[4] + total[5]) * (1.0 / AVG)
    return real - pltpu.roll(imag, 1, 1), imag + pltpu.roll(real, 1, 1)


def spread_flags(flag_ref, block_rows):
    flags = jnp.broadcast_to(flag_ref[...], (8, block_rows)).astype(jnp.float32)
    ahead = lax.broadcasted_iota(jnp.int32, (block_rows, 2 * block_rows), 1)
    ahead = ahead - 2 * lax.broadcasted_iota(jnp.int32, (block_rows, 2 * block_rows), 0)
    hit = jnp.logical_and(ahead >= 0, ahead < 2)
    spread = jnp.where(hit, 1.0, 0.0).astype(jnp.bfloat16)
    return jnp.dot(flags.astype(jnp.bfloat16), spread, preferred_element_type=jnp.float32)


def build_bands(bank_ref, flag_ref, base_ref, band_ref, block_rows):
    out_count, edge, mid, edge_rows, mid_rows, total_rows, period = row_plan(block_rows)
    filters = bank_ref.shape[1]
    to_real, to_imag = spread_taps(bank_ref)
    rest = jnp.zeros((filters, period - to_real.shape[1]), jnp.float32)
    to_real = jnp.concatenate([to_real, rest], axis=1)
    to_imag = pltpu.roll(jnp.concatenate([to_imag, rest], axis=1), period - AVG, 1)
    is_real = lax.broadcasted_iota(jnp.int32, (8, period), 0) % 2 == 0
    for f in range(filters):
        rows = jnp.where(
            is_real,
            jnp.broadcast_to(to_real[f : f + 1], (8, period)),
            jnp.broadcast_to(to_imag[f : f + 1], (8, period)),
        )
        base_ref[f] = pltpu.roll(rows, 0, 1, stride=AVG, stride_axis=0)
    flags = spread_flags(flag_ref, block_rows)
    runs = ((-SIDE, edge, edge_rows), (out_count - SIDE, mid, mid_rows), (SIDE, edge, edge_rows))
    lanes = round_up(2 * block_rows, 128) + 128

    def one_filter(f, carry):
        tile = base_ref[f]
        tiles = []
        for first, count, rows in runs:
            for row in range(0, rows, 8):
                start = (2 * HALF - 2 * AVG * first - AVG * row) % period
                aligned = start // 128 * 128
                piece = jnp.concatenate(
                    [
                        tile[:, at % period : at % period + 128]
                        for at in range(aligned, aligned + lanes, 128)
                    ],
                    axis=1,
                )
                piece = pltpu.roll(piece, (aligned - start) % lanes, 1)[:, : 2 * block_rows]
                piece = piece * flags
                if row + 8 > 2 * count:
                    at = lax.broadcasted_iota(jnp.int32, piece.shape, 0)
                    piece = jnp.where(at < 2 * count - row, piece, 0.0)
                tiles.append(piece)
        band = jnp.concatenate(tiles, axis=0)
        high = band.astype(jnp.bfloat16)
        band_ref[f, :total_rows, :] = high
        band_ref[f, total_rows:, :] = (band - high.astype(jnp.float32)).astype(jnp.bfloat16)
        return carry

    lax.fori_loop(0, filters, one_filter, 0, unroll=2)


def encode(value, code_ref, step_ref, i):
    peak = jnp.max(jnp.max(jnp.abs(value), axis=0, keepdims=True), axis=1, keepdims=True)
    peak = jnp.maximum(peak, TINY)
    step_ref[i : i + 1, :] = jnp.broadcast_to(peak * (1.0 / LEVELS), (1, step_ref.shape[1]))
    code = jnp.round(value * (LEVELS / peak)).astype(jnp.int32).astype(jnp.int16)
    code_ref[:, i] = code.reshape(-1, 2, value.shape[1])


def decode(code):
    rows = code.astype(jnp.int32).astype(jnp.float32)
    return rows.reshape(2 * code.shape[0], code.shape[2])


def stream_kernel(
    index_ref,
    bank_ref,
    flag_ref,
    vis_ref,
    out_ref,
    base_ref,
    band_ref,
    slab_ref,
    sum_ref,
    edge_ref,
    edge_step_ref,
    mid_ref,
    mid_step_ref,
    in_ref,
    in_edge_step_ref,
    in_mid_step_ref,
    done_ref,
    own_ref,
    load_sem,
    edge_send,
    edge_step_send,
    mid_send,
    mid_step_send,
    edge_recv,
    edge_step_recv,
    mid_recv,
    mid_step_recv,
    done_send,
    done_recv,
    own_sem,
    *,
    count,
):
    me = lax.axis_index("tm")
    _, block_rows, group, _, channels = slab_ref.shape
    chunks = done_ref.shape[0]
    per_owner = chunks // count
    out_count, edge, mid, edge_rows, mid_rows, total_rows, _ = row_plan(block_rows)
    alone = out_count - SIDE
    mid_at, far_at = edge_rows, edge_rows + mid_rows
    has_left, has_right = me > 0, me < count - 1
    nearer, farther = jnp.minimum(me, count - 1 - me), jnp.maximum(me, count - 1 - me)
    sign = jnp.where(2 * me <= count - 1, 1, -1)

    def chunk_at(step):
        turn, part = step // per_owner, step % per_owner
        late = turn - (farther - nearer)
        flip = jnp.where(late % 2 == 0, sign, -sign)
        owner = jnp.where(
            late < 0, me + sign * (farther - turn), me + flip * (nearer - late // 2)
        )
        return owner, part, owner * per_owner + part

    def load(step):
        _, _, chunk = chunk_at(step)
        slot = step % LOADS
        return pltpu.make_async_copy(
            vis_ref.at[:, pl.ds(chunk * group, group)], slab_ref.at[slot], load_sem.at[slot]
        )

    def remote(source, target, send_sem, recv_sem, device):
        return pltpu.make_async_remote_copy(
            src_ref=source,
            dst_ref=target,
            send_sem=send_sem,
            recv_sem=recv_sem,
            device_id={"tm": device},
            device_id_type=pl.DeviceIdType.MESH,
        )

    def slot_of(owner, part, chunk, receiver, rightward):
        second = jnp.logical_and(owner == receiver, jnp.logical_not(rightward))
        return jnp.where(second, chunks + part, chunk)

    def edge_copies(chunk, slot, rightward, device):
        start = jnp.where(rightward, mid, 0)
        return (
            remote(
                edge_ref.at[chunk],
                in_ref.at[slot, pl.ds(start, edge)],
                edge_send.at[chunk],
                edge_recv.at[slot],
                device,
            ),
            remote(
                edge_step_ref.at[chunk],
                in_edge_step_ref.at[slot],
                edge_step_send.at[chunk],
                edge_step_recv.at[slot],
                device,
            ),
        )

    def mid_copies(chunk, slot, rightward, device):
        start = jnp.where(rightward, 0, edge)
        return (
            remote(
                mid_ref.at[chunk],
                in_ref.at[slot, pl.ds(start, mid)],
                mid_send.at[chunk],
                mid_recv.at[slot],
                device,
            ),
            remote(
                mid_step_ref.at[chunk],
                in_mid_step_ref.at[slot],
                mid_step_send.at[chunk],
                mid_step_recv.at[slot],
                device,
            ),
        )

    def placed(row, rows, part):
        return out_ref.at[pl.ds(row, rows), pl.ds(part * group, group)]

    def full_done(source, chunk, part, rightward, device):
        row = jnp.where(rightward, out_count * (source - 1) + alone, out_count * source + SIDE)
        return remote(
            done_ref.at[chunk],
            placed(row, edge, part),
            done_send.at[chunk],
            done_recv.at[source, part],
            device,
        )

    def short_done(source, chunk, part, rightward, device):
        row = jnp.where(rightward, 0, out_count * source + SIDE)
        start = jnp.where(rightward, SIDE, 0)
        return remote(
            done_ref.at[chunk, pl.ds(start, alone)],
            placed(row, alone, part),
            done_send.at[chunk],
            done_recv.at[source, part],
            device,
        )

    def keep(part, low, rows):
        return pltpu.make_async_copy(
            own_ref.at[part, pl.ds(low, rows)],
            placed(jnp.maximum(out_count * me - SIDE, 0), rows, part),
            own_sem.at[part],
        )

    for step in range(LOADS - 1):
        load(step).start()
    barrier = pltpu.get_barrier_semaphore()
    for offset in range(1, count):
        pl.semaphore_signal(
            barrier,
            inc=1,
            device_id={"tm": lax.rem(me + offset, count)},
            device_id_type=pl.DeviceIdType.MESH,
        )
    build_bands(bank_ref, flag_ref, base_ref, band_ref, block_rows)
    pl.semaphore_wait(barrier, count - 1)

    def flow(owner):
        rightward = owner > me
        upstream = jnp.where(rightward, has_left, has_right)
        return rightward, upstream, jnp.where(rightward, me + 1, me - 1)

    def compute(step, carry):
        @pl.when(step + LOADS - 1 < chunks)
        def _():
            load(step + LOADS - 1).start()

        load(step).wait()
        owner, part, chunk = chunk_at(step)
        slot = step % LOADS
        rightward, upstream, target = flow(owner)
        landing = slot_of(owner, part, chunk, target, rightward)
        for i in range(group):
            which = index_ref[chunk * group + i]
            slab = slab_ref[slot, :, i].reshape(2 * block_rows, channels)
            both = jnp.dot(band_ref[which], slab, preferred_element_type=jnp.float32)
            sum_ref[chunk, i] = both[:total_rows] + both[total_rows:]

        @pl.when(owner != me)
        def _():
            start = pl.multiple_of(jnp.where(rightward, far_at, 0), 8)
            for i in range(group):
                encode(
                    sum_ref[chunk, i, pl.ds(start, 2 * edge), :],
                    edge_ref.at[chunk],
                    edge_step_ref.at[chunk],
                    i,
                )
            for copy in edge_copies(chunk, landing, rightward, target):
                copy.start()

        @pl.when(jnp.logical_and(owner != me, jnp.logical_not(upstream)))
        def _():
            for i in range(group):
                encode(
                    sum_ref[chunk, i, mid_at : mid_at + 2 * mid, :],
                    mid_ref.at[chunk],
                    mid_step_ref.at[chunk],
                    i,
                )
            for copy in mid_copies(chunk, landing, rightward, target):
                copy.start()

        return carry

    lax.fori_loop(0, chunks, compute, 0)

    def step_of(step_ref, slot, i):
        return jnp.concatenate([step_ref[slot, i : i + 1, :]] * (channels // 128), axis=1)

    def finish(step, carry):
        owner, part, chunk = chunk_at(step)
        rightward, upstream, target = flow(owner)
        landing = slot_of(owner, part, chunk, target, rightward)
        forward = owner != me

        @pl.when(jnp.logical_and(forward, upstream))
        def _():
            for copy in edge_copies(chunk, chunk, rightward, target):
                copy.wait_recv()
            start = jnp.where(rightward, edge, 0)
            for i in range(group):
                came = decode(in_ref[chunk, pl.ds(start, mid), i])
                value = sum_ref[chunk, i, mid_at : mid_at + 2 * mid, :]
                value = value + came * step_of(in_edge_step_ref, chunk, i)
                encode(value, mid_ref.at[chunk], mid_step_ref.at[chunk], i)
            for copy in mid_copies(chunk, landing, rightward, target):
                copy.start()
            for copy in mid_copies(chunk, chunk, rightward, target):
                copy.wait_recv()
            start = jnp.where(rightward, 0, mid)
            near = pl.multiple_of(jnp.where(rightward, 0, far_at), 8)
            at = lax.broadcasted_iota(jnp.int32, (2 * edge, channels), 0)
            first = jnp.where(rightward, 0, 2 * (edge - mid))
            of_mid = jnp.logical_and(at >= first, at < first + 2 * mid)
            for i in range(group):
                came = decode(in_ref[chunk, pl.ds(start, edge), i])
                unit = jnp.where(
                    of_mid,
                    step_of(in_mid_step_ref, chunk, i),
                    step_of(in_edge_step_ref, chunk, i),
                )
                value = sum_ref[chunk, i, pl.ds(near, 2 * edge), :] + came * unit
                done_ref[chunk, :, i] = value.astype(jnp.bfloat16).reshape(edge, 2, channels)
            full_done(me, chunk, part, rightward, owner).start()

        @pl.when(jnp.logical_and(forward, jnp.logical_not(upstream)))
        def _():
            near = pl.multiple_of(jnp.where(rightward, 0, far_at), 8)
            for i in range(group):
                value = sum_ref[chunk, i, pl.ds(near, 2 * edge), :]
                done_ref[chunk, :, i] = value.astype(jnp.bfloat16).reshape(edge, 2, channels)
            short_done(me, chunk, part, rightward, owner).start()

        def from_side(slot, rightward, near, edge_start, first):
            for copy in edge_copies(chunk, slot, rightward, me):
                copy.wait_recv()
            for copy in mid_copies(chunk, slot, rightward, me):
                copy.wait_recv()
            at = lax.broadcasted_iota(jnp.int32, (2 * edge, channels), 0)
            of_mid = jnp.logical_and(at >= first, at < first + 2 * mid)
            for i in range(group):
                edge_unit = step_of(in_edge_step_ref, slot, i)
                unit = jnp.where(of_mid, step_of(in_mid_step_ref, slot, i), edge_unit)
                came = decode(in_ref[slot, edge_start : edge_start + edge, i])
                sum_ref[chunk, i, near : near + 2 * edge, :] += came * unit
                start = edge if rightward else 0
                came = decode(in_ref[slot, start : start + mid, i])
                sum_ref[chunk, i, mid_at : mid_at + 2 * mid, :] += came * edge_unit

        @pl.when(jnp.logical_and(owner == me, has_left))
        def _():
            from_side(chunk, True, 0, 0, 0)

        @pl.when(jnp.logical_and(owner == me, has_right))
        def _():
            from_side(chunks + part, False, far_at, mid, 2 * (edge - mid))

        @pl.when(owner == me)
        def _():
            for i in range(group):
                for row, rows, start in (
                    (0, edge, 0),
                    (edge, mid, mid_at),
                    (edge + mid, edge, far_at),
                ):
                    value = sum_ref[chunk, i, start : start + 2 * rows, :].astype(jnp.bfloat16)
                    own_ref[part, row : row + rows, i] = value.reshape(rows, 2, channels)

            @pl.when(jnp.logical_and(has_left, has_right))
            def _():
                keep(part, 0, 2 * edge + mid).start()

            @pl.when(jnp.logical_not(has_left))
            def _():
                keep(part, SIDE, out_count + SIDE).start()

            @pl.when(jnp.logical_not(has_right))
            def _():
                keep(part, 0, out_count + SIDE).start()

        return carry

    lax.fori_loop(0, chunks, finish, 0)

    def drain(step, carry):
        owner, part, chunk = chunk_at(step)
        rightward, upstream, target = flow(owner)

        @pl.when(owner != me)
        def _():
            for copy in edge_copies(chunk, chunk, rightward, target):
                copy.wait_send()
            for copy in mid_copies(chunk, chunk, rightward, target):
                copy.wait_send()

            @pl.when(upstream)
            def _():
                full_done(me, chunk, part, rightward, owner).wait_send()

            @pl.when(jnp.logical_not(upstream))
            def _():
                short_done(me, chunk, part, rightward, owner).wait_send()

        @pl.when(owner == me)
        def _():
            @pl.when(jnp.logical_and(has_left, has_right))
            def _():
                keep(part, 0, 2 * edge + mid).wait()

            @pl.when(jnp.logical_not(jnp.logical_and(has_left, has_right)))
            def _():
                keep(part, 0, out_count + SIDE).wait()

        return carry

    lax.fori_loop(0, chunks, drain, 0)

    def collect(turn, carry):
        source = lax.rem(me + 1 + turn, count)
        end = jnp.logical_or(source == 0, source == count - 1)
        for part in range(per_owner):

            @pl.when(end)
            def _():
                short_done(source, 0, part, source < me, source).wait_recv()

            @pl.when(jnp.logical_not(end))
            def _():
                full_done(source, 0, part, source < me, source).wait_recv()

        return carry

    lax.fori_loop(0, count - 1, collect, 0)


def stream_call(kernel_index, filter_bank, flags, visibilities):
    block_rows, bases, _, channels = visibilities.shape
    count = lax.axis_size("tm")
    out_count, edge, mid, _, _, total_rows, period = row_plan(block_rows)
    filters = filter_bank.shape[1]
    owned = bases // count
    group = GROUP
    while owned % group:
        group //= 2
    chunks, parts = bases // group, owned // group
    slots = chunks + parts
    sent, landed = pltpu.SemaphoreType.DMA((chunks,)), pltpu.SemaphoreType.DMA((slots,))
    return pl.pallas_call(
        functools.partial(stream_kernel, count=count),
        in_specs=[
            pl.BlockSpec(memory_space=pltpu.SMEM),
            pl.BlockSpec(memory_space=pltpu.VMEM),
            pl.BlockSpec(memory_space=pltpu.VMEM),
            pl.BlockSpec(memory_space=pl.ANY),
        ],
        out_specs=pl.BlockSpec(memory_space=pl.ANY),
        out_shape=jax.ShapeDtypeStruct((count * out_count, owned, 2, channels), jnp.bfloat16),
        scratch_shapes=[
            pltpu.VMEM((filters, 8, period), jnp.float32),
            pltpu.VMEM((filters, 2 * total_rows, 2 * block_rows), jnp.bfloat16),
            pltpu.VMEM((LOADS, block_rows, group, 2, channels), jnp.bfloat16),
            pltpu.VMEM((chunks, group, total_rows, channels), jnp.float32),
            pltpu.VMEM((chunks, edge, group, 2, channels), jnp.int16),
            pltpu.VMEM((chunks, group, 128), jnp.float32),
            pltpu.VMEM((chunks, mid, group, 2, channels), jnp.int16),
            pltpu.VMEM((chunks, group, 128), jnp.float32),
            pltpu.VMEM((slots, edge + mid, group, 2, channels), jnp.int16),
            pltpu.VMEM((slots, group, 128), jnp.float32),
            pltpu.VMEM((slots, group, 128), jnp.float32),
            pltpu.VMEM((chunks, edge, group, 2, channels), jnp.bfloat16),
            pltpu.VMEM((parts, 2 * edge + mid, group, 2, channels), jnp.bfloat16),
            pltpu.SemaphoreType.DMA((LOADS,)),
            sent,
            sent,
            sent,
            sent,
            landed,
            landed,
            landed,
            landed,
            sent,
            pltpu.SemaphoreType.DMA((count, parts)),
            pltpu.SemaphoreType.DMA((parts,)),
        ],
        compiler_params=pltpu.CompilerParams(
            collective_id=0, has_side_effects=True, vmem_limit_bytes=40 * 1024 * 1024
        ),
    )(kernel_index, filter_bank, flags, visibilities)


def per_device(visibilities, flag_mask, kernel_index, filter_bank):
    return stream_call(kernel_index, filter_bank, flag_mask[None, :], visibilities)


def solution(mesh):
    placed = (
        P(("group", "tm"), ("bl", "pol"), None, None),
        P(("group", "tm")),
        P(("bl", "pol")),
        P(),
    )
    return jax.shard_map(
        per_device,
        mesh=mesh,
        in_specs=placed,
        out_specs=P("group", ("bl", "pol", "tm"), None, None),
        check_vma=False,
    )
```

```python
import functools

import jax
import jax.numpy as jnp
from jax import lax
from jax.experimental import pallas as pl
from jax.experimental.pallas import tpu as pltpu
from jax.sharding import PartitionSpec as P

TAPS = 257
AVG = 10
HALF = TAPS // 2
SIDE = -(-HALF // AVG)
GROUP = 8
LOADS = 3
LEVELS = 32767.0
TINY = 1e-33


def round_up(value, step):
    return -(-value // step) * step


def row_plan(block_rows):
    out_count = block_rows // AVG
    edge, mid = out_count, 2 * SIDE - out_count
    assert 0 < mid < SIDE <= out_count
    edge_rows, mid_rows = round_up(2 * edge, 8), round_up(2 * mid, 8)
    total_rows = 2 * edge_rows + mid_rows
    highest = 2 * (block_rows + HALF + AVG * SIDE)
    lowest = 2 * HALF - 2 * AVG * (SIDE + edge)
    period = round_up(max(highest, 2 * (TAPS + AVG) - lowest), 128)
    return out_count, edge, mid, edge_rows, mid_rows, total_rows, period


def tap_spread(taps):
    width = round_up(2 * (taps + AVG), 128)
    ahead = lax.broadcasted_iota(jnp.int32, (taps, width), 1)
    ahead = ahead - 2 * lax.broadcasted_iota(jnp.int32, (taps, width), 0)
    hit = jnp.logical_and(jnp.logical_and(ahead >= 0, ahead < 2 * AVG), ahead % 2 == 0)
    return jnp.where(hit, 1.0, 0.0).astype(jnp.bfloat16)


def spread_taps(bank_ref, spread):
    filters = bank_ref.shape[1]
    parts = []
    for part in (bank_ref[0], bank_ref[1]):
        for _ in range(3):
            parts.append(part.astype(jnp.bfloat16))
            part = part - parts[-1].astype(jnp.float32)
    total = jnp.dot(jnp.concatenate(parts, axis=0), spread, preferred_element_type=jnp.float32)
    total = [total[filters * k : filters * (k + 1)] for k in range(6)]
    real = (total[0] + total[1] + total[2]) * (1.0 / AVG)
    imag = (total[3] + total[4] + total[5]) * (1.0 / AVG)
    return real - pltpu.roll(imag, 1, 1), imag + pltpu.roll(real, 1, 1)


def flag_spread(block_rows):
    ahead = lax.broadcasted_iota(jnp.int32, (block_rows, 2 * block_rows), 1)
    ahead = ahead - 2 * lax.broadcasted_iota(jnp.int32, (block_rows, 2 * block_rows), 0)
    hit = jnp.logical_and(ahead >= 0, ahead < 2)
    return jnp.where(hit, 1.0, 0.0).astype(jnp.bfloat16)


def spread_flags(flag_ref, spread):
    flags = jnp.broadcast_to(flag_ref[...], (8, flag_ref.shape[1])).astype(jnp.float32)
    return jnp.dot(flags.astype(jnp.bfloat16), spread, preferred_element_type=jnp.float32)


def build_bands(bank_ref, flag_ref, base_ref, band_ref, block_rows, copies):
    out_count, edge, mid, edge_rows, mid_rows, total_rows, period = row_plan(block_rows)
    filters = bank_ref.shape[1]
    tap_matrix, flag_matrix = tap_spread(bank_ref.shape[2]), flag_spread(block_rows)
    for copy in copies:
        copy.wait()
    to_real, to_imag = spread_taps(bank_ref, tap_matrix)
    rest = jnp.zeros((filters, period - to_real.shape[1]), jnp.float32)
    to_real = jnp.concatenate([to_real, rest], axis=1)
    to_imag = pltpu.roll(jnp.concatenate([to_imag, rest], axis=1), period - AVG, 1)
    is_real = lax.broadcasted_iota(jnp.int32, (8, period), 0) % 2 == 0
    for f in range(filters):
        rows = jnp.where(
            is_real,
            jnp.broadcast_to(to_real[f : f + 1], (8, period)),
            jnp.broadcast_to(to_imag[f : f + 1], (8, period)),
        )
        base_ref[f] = pltpu.roll(rows, 0, 1, stride=AVG, stride_axis=0)
    flags = spread_flags(flag_ref, flag_matrix)
    runs = ((-SIDE, edge, edge_rows), (out_count - SIDE, mid, mid_rows), (SIDE, edge, edge_rows))
    lanes = round_up(2 * block_rows, 128) + 128

    def one_filter(f, carry):
        tile = base_ref[f]
        tiles = []
        for first, count, rows in runs:
            for row in range(0, rows, 8):
                start = (2 * HALF - 2 * AVG * first - AVG * row) % period
                aligned = start // 128 * 128
                piece = jnp.concatenate(
                    [
                        tile[:, at % period : at % period + 128]
                        for at in range(aligned, aligned + lanes, 128)
                    ],
                    axis=1,
                )
                piece = pltpu.roll(piece, (aligned - start) % lanes, 1)[:, : 2 * block_rows]
                piece = piece * flags
                if row + 8 > 2 * count:
                    at = lax.broadcasted_iota(jnp.int32, piece.shape, 0)
                    piece = jnp.where(at < 2 * count - row, piece, 0.0)
                tiles.append(piece)
        band = jnp.concatenate(tiles, axis=0)
        high = band.astype(jnp.bfloat16)
        band_ref[f, :total_rows, :] = high
        band_ref[f, total_rows:, :] = (band - high.astype(jnp.float32)).astype(jnp.bfloat16)
        return carry

    lax.fori_loop(0, filters, one_filter, 0, unroll=2)


def encode(values, code_ref, step_ref):
    lane = lax.broadcasted_iota(jnp.int32, (1, 128), 1)
    steps = jnp.zeros((1, 128), jnp.float32)
    for i, value in enumerate(values):
        peak = jnp.max(jnp.max(jnp.abs(value), axis=0, keepdims=True), axis=1, keepdims=True)
        peak = jnp.maximum(peak, TINY)
        steps = jnp.where(lane == i, peak * (1.0 / LEVELS), steps)
        code = jnp.round(value * (LEVELS / peak)).astype(jnp.int32).astype(jnp.int16)
        code_ref[:, i] = code.reshape(-1, 2, value.shape[1])
    step_ref[...] = steps


def decode(code):
    rows = code.astype(jnp.int32).astype(jnp.float32)
    return rows.reshape(2 * code.shape[0], code.shape[2])


def stream_kernel(
    index_hbm,
    bank_hbm,
    flag_hbm,
    vis_ref,
    out_ref,
    index_ref,
    bank_ref,
    flag_ref,
    base_ref,
    band_ref,
    slab_ref,
    sum_ref,
    edge_ref,
    edge_step_ref,
    mid_ref,
    mid_step_ref,
    in_ref,
    in_edge_step_ref,
    in_mid_step_ref,
    done_ref,
    own_ref,
    small_sem,
    load_sem,
    edge_send,
    edge_step_send,
    mid_send,
    mid_step_send,
    edge_recv,
    edge_step_recv,
    mid_recv,
    mid_step_recv,
    done_send,
    done_recv,
    own_sem,
    *,
    count,
):
    me = lax.axis_index("tm")
    _, block_rows, group, _, channels = slab_ref.shape
    chunks = done_ref.shape[0]
    per_owner = chunks // count
    out_count, edge, mid, edge_rows, mid_rows, total_rows, _ = row_plan(block_rows)
    alone = out_count - SIDE
    mid_at, far_at = edge_rows, edge_rows + mid_rows
    has_left, has_right = me > 0, me < count - 1
    nearer, farther = jnp.minimum(me, count - 1 - me), jnp.maximum(me, count - 1 - me)
    sign = jnp.where(2 * me <= count - 1, 1, -1)

    def chunk_at(step):
        turn, part = step // per_owner, step % per_owner
        late = turn - (farther - nearer)
        flip = jnp.where(late % 2 == 0, sign, -sign)
        owner = jnp.where(
            late < 0, me + sign * (farther - turn), me + flip * (nearer - late // 2)
        )
        return owner, part, owner * per_owner + part

    def load(step):
        _, _, chunk = chunk_at(step)
        slot = step % LOADS
        return pltpu.make_async_copy(
            vis_ref.at[:, pl.ds(chunk * group, group)], slab_ref.at[slot], load_sem.at[slot]
        )

    def remote(source, target, send_sem, recv_sem, device):
        return pltpu.make_async_remote_copy(
            src_ref=source,
            dst_ref=target,
            send_sem=send_sem,
            recv_sem=recv_sem,
            device_id={"tm": device},
            device_id_type=pl.DeviceIdType.MESH,
        )

    def slot_of(owner, part, chunk, receiver, rightward):
        second = jnp.logical_and(owner == receiver, jnp.logical_not(rightward))
        return jnp.where(second, chunks + part, chunk)

    def edge_copies(chunk, slot, rightward, device):
        start = jnp.where(rightward, mid, 0)
        return (
            remote(
                edge_ref.at[chunk],
                in_ref.at[slot, pl.ds(start, edge)],
                edge_send.at[chunk],
                edge_recv.at[slot],
                device,
            ),
            remote(
                edge_step_ref.at[chunk],
                in_edge_step_ref.at[slot],
                edge_step_send.at[chunk],
                edge_step_recv.at[slot],
                device,
            ),
        )

    def mid_copies(chunk, slot, rightward, device):
        start = jnp.where(rightward, 0, edge)
        return (
            remote(
                mid_ref.at[chunk],
                in_ref.at[slot, pl.ds(start, mid)],
                mid_send.at[chunk],
                mid_recv.at[slot],
                device,
            ),
            remote(
                mid_step_ref.at[chunk],
                in_mid_step_ref.at[slot],
                mid_step_send.at[chunk],
                mid_step_recv.at[slot],
                device,
            ),
        )

    def placed(row, rows, part):
        return out_ref.at[pl.ds(row, rows), pl.ds(part * group, group)]

    def full_done(source, chunk, part, rightward, device):
        row = jnp.where(rightward, out_count * (source - 1) + alone, out_count * source + SIDE)
        return remote(
            done_ref.at[chunk],
            placed(row, edge, part),
            done_send.at[chunk],
            done_recv.at[source, part],
            device,
        )

    def short_done(source, chunk, part, rightward, device):
        row = jnp.where(rightward, 0, out_count * source + SIDE)
        start = jnp.where(rightward, SIDE, 0)
        return remote(
            done_ref.at[chunk, pl.ds(start, alone)],
            placed(row, alone, part),
            done_send.at[chunk],
            done_recv.at[source, part],
            device,
        )

    def keep(part, low, rows):
        return pltpu.make_async_copy(
            own_ref.at[part, pl.ds(low, rows)],
            placed(jnp.maximum(out_count * me - SIDE, 0), rows, part),
            own_sem.at[part],
        )

    smalls = [
        pltpu.make_async_copy(source, target, small_sem.at[k])
        for k, (source, target) in enumerate(
            ((bank_hbm, bank_ref), (flag_hbm, flag_ref), (index_hbm, index_ref))
        )
    ]
    for copy in smalls:
        copy.start()
    for step in range(LOADS - 1):
        load(step).start()
    barrier = pltpu.get_barrier_semaphore()
    for offset in range(1, count):
        pl.semaphore_signal(
            barrier,
            inc=1,
            device_id={"tm": lax.rem(me + offset, count)},
            device_id_type=pl.DeviceIdType.MESH,
        )
    build_bands(bank_ref, flag_ref, base_ref, band_ref, block_rows, smalls)
    pl.semaphore_wait(barrier, count - 1)

    def flow(owner):
        rightward = owner > me
        upstream = jnp.where(rightward, has_left, has_right)
        return rightward, upstream, jnp.where(rightward, me + 1, me - 1)

    def compute(step, carry):
        @pl.when(step + LOADS - 1 < chunks)
        def _():
            load(step + LOADS - 1).start()

        load(step).wait()
        owner, part, chunk = chunk_at(step)
        slot = step % LOADS
        rightward, upstream, target = flow(owner)
        landing = slot_of(owner, part, chunk, target, rightward)
        for i in range(group):
            which = index_ref[chunk * group + i]
            slab = slab_ref[slot, :, i].reshape(2 * block_rows, channels)
            both = jnp.dot(band_ref[which], slab, preferred_element_type=jnp.float32)
            sum_ref[chunk, i] = both[:total_rows] + both[total_rows:]

        @pl.when(owner != me)
        def _():
            start = pl.multiple_of(jnp.where(rightward, far_at, 0), 8)
            values = [sum_ref[chunk, i, pl.ds(start, 2 * edge), :] for i in range(group)]
            encode(values, edge_ref.at[chunk], edge_step_ref.at[chunk])
            for copy in edge_copies(chunk, landing, rightward, target):
                copy.start()

        ends = jnp.logical_and(owner != me, jnp.logical_not(upstream))

        @pl.when(ends)
        def _():
            values = [sum_ref[chunk, i, mid_at : mid_at + 2 * mid, :] for i in range(group)]
            encode(values, mid_ref.at[chunk], mid_step_ref.at[chunk])

        turn = step // per_owner
        paired = jnp.logical_or(turn % 2 == 1, turn == count - 2)
        paired = jnp.logical_and(paired, part == per_owner - 1)

        @pl.when(jnp.logical_and(ends, paired))
        def _():
            def start_mid(back, carry):
                owner, part, chunk = chunk_at(back)
                rightward, _, target = flow(owner)
                landing = slot_of(owner, part, chunk, target, rightward)
                for copy in mid_copies(chunk, landing, rightward, target):
                    copy.start()
                return carry

            lax.fori_loop((turn - turn % 2) * per_owner, step + 1, start_mid, 0)

        return carry

    lax.fori_loop(0, chunks, compute, 0)
    forward = chunks - per_owner

    def came(slot, start, rows, i):
        return decode(in_ref[slot, pl.ds(start, rows), i])

    def pass_mid(step, carry):
        owner, part, chunk = chunk_at(step)
        rightward, upstream, target = flow(owner)
        landing = slot_of(owner, part, chunk, target, rightward)

        @pl.when(upstream)
        def _():
            for copy in edge_copies(chunk, chunk, rightward, target):
                copy.wait_recv()
            start = jnp.where(rightward, edge, 0)
            units = in_edge_step_ref[chunk]
            values = [
                sum_ref[chunk, i, mid_at : mid_at + 2 * mid, :]
                + came(chunk, start, mid, i) * units[:, i : i + 1]
                for i in range(group)
            ]
            encode(values, mid_ref.at[chunk], mid_step_ref.at[chunk])
            for copy in mid_copies(chunk, landing, rightward, target):
                copy.start()

        return carry

    lax.fori_loop(0, forward, pass_mid, 0)

    def round_off(value, rows):
        return value.astype(jnp.bfloat16).reshape(rows, 2, channels)

    def pass_done(step, carry):
        owner, part, chunk = chunk_at(step)
        rightward, upstream, target = flow(owner)
        near = pl.multiple_of(jnp.where(rightward, 0, far_at), 8)

        @pl.when(upstream)
        def _():
            for copy in mid_copies(chunk, chunk, rightward, target):
                copy.wait_recv()
            start = jnp.where(rightward, 0, mid)
            at = lax.broadcasted_iota(jnp.int32, (2 * edge, channels), 0)
            first = jnp.where(rightward, 0, 2 * (edge - mid))
            of_mid = jnp.logical_and(at >= first, at < first + 2 * mid)
            mids, edges = in_mid_step_ref[chunk], in_edge_step_ref[chunk]
            for i in range(group):
                unit = jnp.where(of_mid, mids[:, i : i + 1], edges[:, i : i + 1])
                value = sum_ref[chunk, i, pl.ds(near, 2 * edge), :]
                value = value + came(chunk, start, edge, i) * unit
                done_ref[chunk, :, i] = round_off(value, edge)
            full_done(me, chunk, part, rightward, owner).start()

        @pl.when(jnp.logical_not(upstream))
        def _():
            for i in range(group):
                value = sum_ref[chunk, i, pl.ds(near, 2 * edge), :]
                done_ref[chunk, :, i] = round_off(value, edge)
            short_done(me, chunk, part, rightward, owner).start()

        return carry

    lax.fori_loop(0, forward, pass_done, 0)

    def pass_own(part, carry):
        chunk = me * per_owner + part

        def from_side(slot, rightward, near, edge_start, first):
            for copy in edge_copies(chunk, slot, rightward, me):
                copy.wait_recv()
            for copy in mid_copies(chunk, slot, rightward, me):
                copy.wait_recv()
            at = lax.broadcasted_iota(jnp.int32, (2 * edge, channels), 0)
            of_mid = jnp.logical_and(at >= first, at < first + 2 * mid)
            mids, edges = in_mid_step_ref[slot], in_edge_step_ref[slot]
            start = edge if rightward else 0
            for i in range(group):
                unit = jnp.where(of_mid, mids[:, i : i + 1], edges[:, i : i + 1])
                sum_ref[chunk, i, near : near + 2 * edge, :] += (
                    came(slot, edge_start, edge, i) * unit
                )
                sum_ref[chunk, i, mid_at : mid_at + 2 * mid, :] += (
                    came(slot, start, mid, i) * edges[:, i : i + 1]
                )

        @pl.when(has_left)
        def _():
            from_side(chunk, True, 0, 0, 0)

        @pl.when(has_right)
        def _():
            from_side(chunks + part, False, far_at, mid, 2 * (edge - mid))

        for i in range(group):
            for row, rows, start in (
                (0, edge, 0),
                (edge, mid, mid_at),
                (edge + mid, edge, far_at),
            ):
                value = sum_ref[chunk, i, start : start + 2 * rows, :]
                own_ref[part, row : row + rows, i] = round_off(value, rows)

        @pl.when(jnp.logical_and(has_left, has_right))
        def _():
            keep(part, 0, 2 * edge + mid).start()

        @pl.when(jnp.logical_not(has_left))
        def _():
            keep(part, SIDE, out_count + SIDE).start()

        @pl.when(jnp.logical_not(has_right))
        def _():
            keep(part, 0, out_count + SIDE).start()

        return carry

    lax.fori_loop(0, per_owner, pass_own, 0)

    def drain(step, carry):
        owner, part, chunk = chunk_at(step)
        rightward, upstream, target = flow(owner)

        @pl.when(owner != me)
        def _():
            for copy in edge_copies(chunk, chunk, rightward, target):
                copy.wait_send()
            for copy in mid_copies(chunk, chunk, rightward, target):
                copy.wait_send()

            @pl.when(upstream)
            def _():
                full_done(me, chunk, part, rightward, owner).wait_send()

            @pl.when(jnp.logical_not(upstream))
            def _():
                short_done(me, chunk, part, rightward, owner).wait_send()

        @pl.when(owner == me)
        def _():
            @pl.when(jnp.logical_and(has_left, has_right))
            def _():
                keep(part, 0, 2 * edge + mid).wait()

            @pl.when(jnp.logical_not(jnp.logical_and(has_left, has_right)))
            def _():
                keep(part, 0, out_count + SIDE).wait()

        return carry

    lax.fori_loop(0, chunks, drain, 0)

    def collect(turn, carry):
        source = lax.rem(me + 1 + turn, count)
        end = jnp.logical_or(source == 0, source == count - 1)
        for part in range(per_owner):

            @pl.when(end)
            def _():
                short_done(source, 0, part, source < me, source).wait_recv()

            @pl.when(jnp.logical_not(end))
            def _():
                full_done(source, 0, part, source < me, source).wait_recv()

        return carry

    lax.fori_loop(0, count - 1, collect, 0)


def stream_call(kernel_index, filter_bank, flags, visibilities):
    block_rows, bases, _, channels = visibilities.shape
    count = lax.axis_size("tm")
    out_count, edge, mid, _, _, total_rows, period = row_plan(block_rows)
    filters = filter_bank.shape[1]
    owned = bases // count
    group = GROUP
    while owned % group:
        group //= 2
    chunks, parts = bases // group, owned // group
    slots = chunks + parts
    small = [
        pltpu.with_memory_space_constraint(operand, pltpu.HBM)
        for operand in (kernel_index, filter_bank, flags)
    ]
    sent, landed = pltpu.SemaphoreType.DMA((chunks,)), pltpu.SemaphoreType.DMA((slots,))
    return pl.pallas_call(
        functools.partial(stream_kernel, count=count),
        in_specs=[
            pl.BlockSpec(memory_space=pltpu.HBM),
            pl.BlockSpec(memory_space=pltpu.HBM),
            pl.BlockSpec(memory_space=pltpu.HBM),
            pl.BlockSpec(memory_space=pl.ANY),
        ],
        out_specs=pl.BlockSpec(memory_space=pl.ANY),
        out_shape=jax.ShapeDtypeStruct((count * out_count, owned, 2, channels), jnp.bfloat16),
        scratch_shapes=[
            pltpu.SMEM(kernel_index.shape, jnp.int32),
            pltpu.VMEM(filter_bank.shape, jnp.float32),
            pltpu.VMEM(flags.shape, jnp.int32),
            pltpu.VMEM((filters, 8, period), jnp.float32),
            pltpu.VMEM((filters, 2 * total_rows, 2 * block_rows), jnp.bfloat16),
            pltpu.VMEM((LOADS, block_rows, group, 2, channels), jnp.bfloat16),
            pltpu.VMEM((chunks, group, total_rows, channels), jnp.float32),
            pltpu.VMEM((chunks, edge, group, 2, channels), jnp.int16),
            pltpu.VMEM((chunks, 1, 128), jnp.float32),
            pltpu.VMEM((chunks, mid, group, 2, channels), jnp.int16),
            pltpu.VMEM((chunks, 1, 128), jnp.float32),
            pltpu.VMEM((slots, edge + mid, group, 2, channels), jnp.int16),
            pltpu.VMEM((slots, 1, 128), jnp.float32),
            pltpu.VMEM((slots, 1, 128), jnp.float32),
            pltpu.VMEM((chunks, edge, group, 2, channels), jnp.bfloat16),
            pltpu.VMEM((parts, 2 * edge + mid, group, 2, channels), jnp.bfloat16),
            pltpu.SemaphoreType.DMA((3,)),
            pltpu.SemaphoreType.DMA((LOADS,)),
            sent,
            sent,
            sent,
            sent,
            landed,
            landed,
            landed,
            landed,
            sent,
            pltpu.SemaphoreType.DMA((count, parts)),
            pltpu.SemaphoreType.DMA((parts,)),
        ],
        compiler_params=pltpu.CompilerParams(
            collective_id=0, has_side_effects=True, vmem_limit_bytes=40 * 1024 * 1024
        ),
    )(*small, visibilities)


def per_device(visibilities, flag_mask, kernel_index, filter_bank):
    return stream_call(kernel_index, filter_bank, flag_mask[None, :], visibilities)


def solution(mesh):
    placed = (
        P(("group", "tm"), ("bl", "pol"), None, None),
        P(("group", "tm")),
        P(("bl", "pol")),
        P(),
    )
    return jax.shard_map(
        per_device,
        mesh=mesh,
        in_specs=placed,
        out_specs=P("group", ("bl", "pol", "tm"), None, None),
        check_vma=False,
    )
```

```python
import functools

import jax
import jax.numpy as jnp
from jax import lax
from jax.experimental import pallas as pl
from jax.experimental.pallas import tpu as pltpu
from jax.sharding import PartitionSpec as P

TAPS = 257
AVG = 10
HALF = TAPS // 2
SIDE = -(-HALF // AVG)
GROUP = 8
LOADS = 3
LEVELS = 32767.0
TINY = 1e-33


def round_up(value, step):
    return -(-value // step) * step


def row_plan(block_rows):
    out_count = block_rows // AVG
    edge, mid = out_count, 2 * SIDE - out_count
    assert 0 < mid < SIDE <= out_count
    edge_rows, mid_rows = round_up(2 * edge, 8), round_up(2 * mid, 8)
    total_rows = 2 * edge_rows + mid_rows
    highest = 2 * (block_rows + HALF + AVG * SIDE)
    lowest = 2 * HALF - 2 * AVG * (SIDE + edge)
    period = round_up(max(highest, 2 * (TAPS + AVG) - lowest), 128)
    return out_count, edge, mid, edge_rows, mid_rows, total_rows, period


def tap_spread(taps):
    width = round_up(2 * (taps + AVG), 128)
    ahead = lax.broadcasted_iota(jnp.int32, (taps, width), 1)
    ahead = ahead - 2 * lax.broadcasted_iota(jnp.int32, (taps, width), 0)
    hit = jnp.logical_and(jnp.logical_and(ahead >= 0, ahead < 2 * AVG), ahead % 2 == 0)
    return jnp.where(hit, 1.0, 0.0).astype(jnp.bfloat16)


def spread_taps(bank_ref, spread):
    filters = bank_ref.shape[1]
    parts = []
    for part in (bank_ref[0], bank_ref[1]):
        for _ in range(3):
            parts.append(part.astype(jnp.bfloat16))
            part = part - parts[-1].astype(jnp.float32)
    total = jnp.dot(jnp.concatenate(parts, axis=0), spread, preferred_element_type=jnp.float32)
    total = [total[filters * k : filters * (k + 1)] for k in range(6)]
    real = (total[0] + total[1] + total[2]) * (1.0 / AVG)
    imag = (total[3] + total[4] + total[5]) * (1.0 / AVG)
    return real - pltpu.roll(imag, 1, 1), imag + pltpu.roll(real, 1, 1)


def flag_spread(block_rows):
    ahead = lax.broadcasted_iota(jnp.int32, (block_rows, 2 * block_rows), 1)
    ahead = ahead - 2 * lax.broadcasted_iota(jnp.int32, (block_rows, 2 * block_rows), 0)
    hit = jnp.logical_and(ahead >= 0, ahead < 2)
    return jnp.where(hit, 1.0, 0.0).astype(jnp.bfloat16)


def spread_flags(flag_ref, spread):
    flags = jnp.broadcast_to(flag_ref[...], (8, flag_ref.shape[1])).astype(jnp.float32)
    return jnp.dot(flags.astype(jnp.bfloat16), spread, preferred_element_type=jnp.float32)


def build_rows(bank_ref, flag_ref, real_ref, imag_ref, good_ref, block_rows, copies):
    period = row_plan(block_rows)[6]
    tap_matrix, flag_matrix = tap_spread(bank_ref.shape[2]), flag_spread(block_rows)
    for copy in copies:
        copy.wait()
    to_real, to_imag = spread_taps(bank_ref, tap_matrix)
    rest = jnp.zeros((to_real.shape[0], period - to_real.shape[1]), jnp.float32)
    real_ref[...] = jnp.concatenate([to_real, rest], axis=1)
    imag_ref[...] = pltpu.roll(jnp.concatenate([to_imag, rest], axis=1), period - AVG, 1)
    good_ref[...] = spread_flags(flag_ref, flag_matrix)


def build_band(real, imag, flags, block_rows):
    out_count, edge, mid, edge_rows, mid_rows, total_rows, period = row_plan(block_rows)
    is_real = lax.broadcasted_iota(jnp.int32, (8, period), 0) % 2 == 0
    tile = jnp.where(
        is_real, jnp.broadcast_to(real, (8, period)), jnp.broadcast_to(imag, (8, period))
    )
    tile = pltpu.roll(tile, 0, 1, stride=AVG, stride_axis=0)
    runs = ((-SIDE, edge, edge_rows), (out_count - SIDE, mid, mid_rows), (SIDE, edge, edge_rows))
    lanes = round_up(2 * block_rows, 128) + 128
    tiles = []
    for first, count, rows in runs:
        for row in range(0, rows, 8):
            start = (2 * HALF - 2 * AVG * first - AVG * row) % period
            aligned = start // 128 * 128
            piece = jnp.concatenate(
                [
                    tile[:, at % period : at % period + 128]
                    for at in range(aligned, aligned + lanes, 128)
                ],
                axis=1,
            )
            piece = pltpu.roll(piece, (aligned - start) % lanes, 1)[:, : 2 * block_rows]
            piece = piece * flags
            if row + 8 > 2 * count:
                at = lax.broadcasted_iota(jnp.int32, piece.shape, 0)
                piece = jnp.where(at < 2 * count - row, piece, 0.0)
            tiles.append(piece)
    band = jnp.concatenate(tiles, axis=0)
    high = band.astype(jnp.bfloat16)
    low = (band - high.astype(jnp.float32)).astype(jnp.bfloat16)
    return jnp.concatenate([high, low], axis=0)


def encode(values, code_ref, step_ref):
    lane = lax.broadcasted_iota(jnp.int32, (1, 128), 1)
    steps = jnp.zeros((1, 128), jnp.float32)
    for i, value in enumerate(values):
        peak = jnp.max(jnp.max(jnp.abs(value), axis=0, keepdims=True), axis=1, keepdims=True)
        peak = jnp.maximum(peak, TINY)
        steps = jnp.where(lane == i, peak * (1.0 / LEVELS), steps)
        code = jnp.round(value * (LEVELS / peak)).astype(jnp.int32).astype(jnp.int16)
        code_ref[:, i] = code.reshape(-1, 2, value.shape[1])
    step_ref[...] = steps


def decode(code):
    rows = code.astype(jnp.int32).astype(jnp.float32)
    return rows.reshape(2 * code.shape[0], code.shape[2])


def stream_kernel(
    index_hbm,
    bank_hbm,
    flag_hbm,
    vis_ref,
    out_ref,
    index_ref,
    bank_ref,
    flag_ref,
    real_ref,
    imag_ref,
    good_ref,
    slab_ref,
    sum_ref,
    edge_ref,
    edge_step_ref,
    mid_ref,
    mid_step_ref,
    in_ref,
    in_edge_step_ref,
    in_mid_step_ref,
    done_ref,
    own_ref,
    small_sem,
    load_sem,
    edge_send,
    edge_step_send,
    mid_send,
    mid_step_send,
    edge_recv,
    edge_step_recv,
    mid_recv,
    mid_step_recv,
    done_send,
    done_recv,
    own_sem,
    *,
    count,
):
    me = lax.axis_index("tm")
    _, block_rows, group, _, channels = slab_ref.shape
    chunks = done_ref.shape[0]
    per_owner = chunks // count
    out_count, edge, mid, edge_rows, mid_rows, total_rows, _ = row_plan(block_rows)
    alone = out_count - SIDE
    mid_at, far_at = edge_rows, edge_rows + mid_rows
    has_left, has_right = me > 0, me < count - 1
    nearer, farther = jnp.minimum(me, count - 1 - me), jnp.maximum(me, count - 1 - me)
    sign = jnp.where(2 * me <= count - 1, 1, -1)

    def chunk_at(step):
        turn, part = step // per_owner, step % per_owner
        late = turn - (farther - nearer)
        flip = jnp.where(late % 2 == 0, sign, -sign)
        owner = jnp.where(
            late < 0, me + sign * (farther - turn), me + flip * (nearer - late // 2)
        )
        return owner, part, owner * per_owner + part

    pieces = load_sem.shape[1]
    share = group // pieces

    def load(step, piece):
        _, _, chunk = chunk_at(step)
        slot = step % LOADS
        return pltpu.make_async_copy(
            vis_ref.at[:, pl.ds(chunk * group + piece * share, share)],
            slab_ref.at[slot, :, pl.ds(piece * share, share)],
            load_sem.at[slot, piece],
        )

    def remote(source, target, send_sem, recv_sem, device):
        return pltpu.make_async_remote_copy(
            src_ref=source,
            dst_ref=target,
            send_sem=send_sem,
            recv_sem=recv_sem,
            device_id={"tm": device},
            device_id_type=pl.DeviceIdType.MESH,
        )

    def slot_of(owner, part, chunk, receiver, rightward):
        second = jnp.logical_and(owner == receiver, jnp.logical_not(rightward))
        return jnp.where(second, chunks + part, chunk)

    def edge_copies(chunk, slot, rightward, device):
        start = jnp.where(rightward, mid, 0)
        return (
            remote(
                edge_ref.at[chunk],
                in_ref.at[slot, pl.ds(start, edge)],
                edge_send.at[chunk],
                edge_recv.at[slot],
                device,
            ),
            remote(
                edge_step_ref.at[chunk],
                in_edge_step_ref.at[slot],
                edge_step_send.at[chunk],
                edge_step_recv.at[slot],
                device,
            ),
        )

    def mid_copies(chunk, slot, rightward, device):
        start = jnp.where(rightward, 0, edge)
        return (
            remote(
                mid_ref.at[chunk],
                in_ref.at[slot, pl.ds(start, mid)],
                mid_send.at[chunk],
                mid_recv.at[slot],
                device,
            ),
            remote(
                mid_step_ref.at[chunk],
                in_mid_step_ref.at[slot],
                mid_step_send.at[chunk],
                mid_step_recv.at[slot],
                device,
            ),
        )

    def placed(row, rows, part):
        return out_ref.at[pl.ds(row, rows), pl.ds(part * group, group)]

    def full_done(source, chunk, part, rightward, device):
        row = jnp.where(rightward, out_count * (source - 1) + alone, out_count * source + SIDE)
        return remote(
            done_ref.at[chunk],
            placed(row, edge, part),
            done_send.at[chunk],
            done_recv.at[source, part],
            device,
        )

    def short_done(source, chunk, part, rightward, device):
        row = jnp.where(rightward, 0, out_count * source + SIDE)
        start = jnp.where(rightward, SIDE, 0)
        return remote(
            done_ref.at[chunk, pl.ds(start, alone)],
            placed(row, alone, part),
            done_send.at[chunk],
            done_recv.at[source, part],
            device,
        )

    def keep(part, low, rows):
        return pltpu.make_async_copy(
            own_ref.at[part, pl.ds(low, rows)],
            placed(jnp.maximum(out_count * me - SIDE, 0), rows, part),
            own_sem.at[part],
        )

    smalls = [
        pltpu.make_async_copy(source, target, small_sem.at[k])
        for k, (source, target) in enumerate(
            ((bank_hbm, bank_ref), (flag_hbm, flag_ref), (index_hbm, index_ref))
        )
    ]
    for copy in smalls:
        copy.start()
    for piece in range(pieces):
        load(0, piece).start()
    barrier = pltpu.get_barrier_semaphore()
    for offset in range(1, count):
        pl.semaphore_signal(
            barrier,
            inc=1,
            device_id={"tm": lax.rem(me + offset, count)},
            device_id_type=pl.DeviceIdType.MESH,
        )
    build_rows(bank_ref, flag_ref, real_ref, imag_ref, good_ref, block_rows, smalls)
    for step in range(1, LOADS - 1):
        for piece in range(pieces):
            load(step, piece).start()
    pl.semaphore_wait(barrier, count - 1)

    def flow(owner):
        rightward = owner > me
        upstream = jnp.where(rightward, has_left, has_right)
        return rightward, upstream, jnp.where(rightward, me + 1, me - 1)

    def compute(step, carry):
        @pl.when(step + LOADS - 1 < chunks)
        def _():
            for piece in range(pieces):
                load(step + LOADS - 1, piece).start()

        owner, part, chunk = chunk_at(step)
        slot = step % LOADS
        rightward, upstream, target = flow(owner)
        landing = slot_of(owner, part, chunk, target, rightward)
        for i in range(group):
            if i % share == 0:
                load(step, i // share).wait()
            which = index_ref[chunk * group + i]
            real, imag = real_ref[pl.ds(which, 1), :], imag_ref[pl.ds(which, 1), :]
            band = build_band(real, imag, good_ref[...], block_rows)
            slab = slab_ref[slot, :, i].reshape(2 * block_rows, channels)
            both = jnp.dot(band, slab, preferred_element_type=jnp.float32)
            sum_ref[chunk, i] = both[:total_rows] + both[total_rows:]

        @pl.when(owner != me)
        def _():
            start = pl.multiple_of(jnp.where(rightward, far_at, 0), 8)
            values = [sum_ref[chunk, i, pl.ds(start, 2 * edge), :] for i in range(group)]
            encode(values, edge_ref.at[chunk], edge_step_ref.at[chunk])
            for copy in edge_copies(chunk, landing, rightward, target):
                copy.start()

        ends = jnp.logical_and(owner != me, jnp.logical_not(upstream))

        @pl.when(ends)
        def _():
            values = [sum_ref[chunk, i, mid_at : mid_at + 2 * mid, :] for i in range(group)]
            encode(values, mid_ref.at[chunk], mid_step_ref.at[chunk])

        turn = step // per_owner
        paired = jnp.logical_or(turn % 2 == 1, turn == count - 2)
        paired = jnp.logical_and(paired, part == per_owner - 1)

        @pl.when(jnp.logical_and(ends, paired))
        def _():
            def start_mid(back, carry):
                owner, part, chunk = chunk_at(back)
                rightward, _, target = flow(owner)
                landing = slot_of(owner, part, chunk, target, rightward)
                for copy in mid_copies(chunk, landing, rightward, target):
                    copy.start()
                return carry

            lax.fori_loop((turn - turn % 2) * per_owner, step + 1, start_mid, 0)

        return carry

    lax.fori_loop(0, chunks, compute, 0)
    forward = chunks - per_owner

    def came(slot, start, rows, i):
        return decode(in_ref[slot, pl.ds(start, rows), i])

    def pass_mid(step, carry):
        owner, part, chunk = chunk_at(step)
        rightward, upstream, target = flow(owner)
        landing = slot_of(owner, part, chunk, target, rightward)

        @pl.when(upstream)
        def _():
            for copy in edge_copies(chunk, chunk, rightward, target):
                copy.wait_recv()
            start = jnp.where(rightward, edge, 0)
            units = in_edge_step_ref[chunk]
            values = [
                sum_ref[chunk, i, mid_at : mid_at + 2 * mid, :]
                + came(chunk, start, mid, i) * units[:, i : i + 1]
                for i in range(group)
            ]
            encode(values, mid_ref.at[chunk], mid_step_ref.at[chunk])
            for copy in mid_copies(chunk, landing, rightward, target):
                copy.start()

        return carry

    lax.fori_loop(0, forward, pass_mid, 0)

    def round_off(value, rows):
        return value.astype(jnp.bfloat16).reshape(rows, 2, channels)

    def pass_done(step, carry):
        owner, part, chunk = chunk_at(step)
        rightward, upstream, target = flow(owner)
        near = pl.multiple_of(jnp.where(rightward, 0, far_at), 8)

        @pl.when(upstream)
        def _():
            for copy in mid_copies(chunk, chunk, rightward, target):
                copy.wait_recv()
            start = jnp.where(rightward, 0, mid)
            at = lax.broadcasted_iota(jnp.int32, (2 * edge, channels), 0)
            first = jnp.where(rightward, 0, 2 * (edge - mid))
            of_mid = jnp.logical_and(at >= first, at < first + 2 * mid)
            mids, edges = in_mid_step_ref[chunk], in_edge_step_ref[chunk]
            for i in range(group):
                unit = jnp.where(of_mid, mids[:, i : i + 1], edges[:, i : i + 1])
                value = sum_ref[chunk, i, pl.ds(near, 2 * edge), :]
                value = value + came(chunk, start, edge, i) * unit
                done_ref[chunk, :, i] = round_off(value, edge)
            full_done(me, chunk, part, rightward, owner).start()

        @pl.when(jnp.logical_not(upstream))
        def _():
            for i in range(group):
                value = sum_ref[chunk, i, pl.ds(near, 2 * edge), :]
                done_ref[chunk, :, i] = round_off(value, edge)
            short_done(me, chunk, part, rightward, owner).start()

        return carry

    lax.fori_loop(0, forward, pass_done, 0)

    def pass_own(part, carry):
        chunk = me * per_owner + part

        def from_side(slot, rightward, near, edge_start, first):
            for copy in edge_copies(chunk, slot, rightward, me):
                copy.wait_recv()
            for copy in mid_copies(chunk, slot, rightward, me):
                copy.wait_recv()
            at = lax.broadcasted_iota(jnp.int32, (2 * edge, channels), 0)
            of_mid = jnp.logical_and(at >= first, at < first + 2 * mid)
            mids, edges = in_mid_step_ref[slot], in_edge_step_ref[slot]
            start = edge if rightward else 0
            for i in range(group):
                unit = jnp.where(of_mid, mids[:, i : i + 1], edges[:, i : i + 1])
                sum_ref[chunk, i, near : near + 2 * edge, :] += (
                    came(slot, edge_start, edge, i) * unit
                )
                sum_ref[chunk, i, mid_at : mid_at + 2 * mid, :] += (
                    came(slot, start, mid, i) * edges[:, i : i + 1]
                )

        @pl.when(has_left)
        def _():
            from_side(chunk, True, 0, 0, 0)

        @pl.when(has_right)
        def _():
            from_side(chunks + part, False, far_at, mid, 2 * (edge - mid))

        for i in range(group):
            for row, rows, start in (
                (0, edge, 0),
                (edge, mid, mid_at),
                (edge + mid, edge, far_at),
            ):
                value = sum_ref[chunk, i, start : start + 2 * rows, :]
                own_ref[part, row : row + rows, i] = round_off(value, rows)

        @pl.when(jnp.logical_and(has_left, has_right))
        def _():
            keep(part, 0, 2 * edge + mid).start()

        @pl.when(jnp.logical_not(has_left))
        def _():
            keep(part, SIDE, out_count + SIDE).start()

        @pl.when(jnp.logical_not(has_right))
        def _():
            keep(part, 0, out_count + SIDE).start()

        return carry

    lax.fori_loop(0, per_owner, pass_own, 0)

    def drain(step, carry):
        owner, part, chunk = chunk_at(step)
        rightward, upstream, target = flow(owner)

        @pl.when(owner != me)
        def _():
            for copy in edge_copies(chunk, chunk, rightward, target):
                copy.wait_send()
            for copy in mid_copies(chunk, chunk, rightward, target):
                copy.wait_send()

            @pl.when(upstream)
            def _():
                full_done(me, chunk, part, rightward, owner).wait_send()

            @pl.when(jnp.logical_not(upstream))
            def _():
                short_done(me, chunk, part, rightward, owner).wait_send()

        @pl.when(owner == me)
        def _():
            @pl.when(jnp.logical_and(has_left, has_right))
            def _():
                keep(part, 0, 2 * edge + mid).wait()

            @pl.when(jnp.logical_not(jnp.logical_and(has_left, has_right)))
            def _():
                keep(part, 0, out_count + SIDE).wait()

        return carry

    lax.fori_loop(0, chunks, drain, 0)

    def collect(turn, carry):
        source = lax.rem(me + 1 + turn, count)
        end = jnp.logical_or(source == 0, source == count - 1)
        for part in range(per_owner):

            @pl.when(end)
            def _():
                short_done(source, 0, part, source < me, source).wait_recv()

            @pl.when(jnp.logical_not(end))
            def _():
                full_done(source, 0, part, source < me, source).wait_recv()

        return carry

    lax.fori_loop(0, count - 1, collect, 0)


def stream_call(kernel_index, filter_bank, flags, visibilities):
    block_rows, bases, _, channels = visibilities.shape
    count = lax.axis_size("tm")
    out_count, edge, mid, _, _, total_rows, period = row_plan(block_rows)
    filters = filter_bank.shape[1]
    owned = bases // count
    group = GROUP
    while owned % group:
        group //= 2
    chunks, parts = bases // group, owned // group
    slots = chunks + parts
    small = [
        pltpu.with_memory_space_constraint(operand, pltpu.HBM)
        for operand in (kernel_index, filter_bank, flags)
    ]
    sent, landed = pltpu.SemaphoreType.DMA((chunks,)), pltpu.SemaphoreType.DMA((slots,))
    return pl.pallas_call(
        functools.partial(stream_kernel, count=count),
        in_specs=[
            pl.BlockSpec(memory_space=pltpu.HBM),
            pl.BlockSpec(memory_space=pltpu.HBM),
            pl.BlockSpec(memory_space=pltpu.HBM),
            pl.BlockSpec(memory_space=pl.ANY),
        ],
        out_specs=pl.BlockSpec(memory_space=pl.ANY),
        out_shape=jax.ShapeDtypeStruct((count * out_count, owned, 2, channels), jnp.bfloat16),
        scratch_shapes=[
            pltpu.SMEM(kernel_index.shape, jnp.int32),
            pltpu.VMEM(filter_bank.shape, jnp.float32),
            pltpu.VMEM(flags.shape, jnp.int32),
            pltpu.VMEM((filters, period), jnp.float32),
            pltpu.VMEM((filters, period), jnp.float32),
            pltpu.VMEM((8, 2 * block_rows), jnp.float32),
            pltpu.VMEM((LOADS, block_rows, group, 2, channels), jnp.bfloat16),
            pltpu.VMEM((chunks, group, total_rows, channels), jnp.float32),
            pltpu.VMEM((chunks, edge, group, 2, channels), jnp.int16),
            pltpu.VMEM((chunks, 1, 128), jnp.float32),
            pltpu.VMEM((chunks, mid, group, 2, channels), jnp.int16),
            pltpu.VMEM((chunks, 1, 128), jnp.float32),
            pltpu.VMEM((slots, edge + mid, group, 2, channels), jnp.int16),
            pltpu.VMEM((slots, 1, 128), jnp.float32),
            pltpu.VMEM((slots, 1, 128), jnp.float32),
            pltpu.VMEM((chunks, edge, group, 2, channels), jnp.bfloat16),
            pltpu.VMEM((parts, 2 * edge + mid, group, 2, channels), jnp.bfloat16),
            pltpu.SemaphoreType.DMA((3,)),
            pltpu.SemaphoreType.DMA((LOADS, 2 if group % 2 == 0 else 1)),
            sent,
            sent,
            sent,
            sent,
            landed,
            landed,
            landed,
            landed,
            sent,
            pltpu.SemaphoreType.DMA((count, parts)),
            pltpu.SemaphoreType.DMA((parts,)),
        ],
        compiler_params=pltpu.CompilerParams(
            collective_id=0, has_side_effects=True, vmem_limit_bytes=40 * 1024 * 1024
        ),
    )(*small, visibilities)


def per_device(visibilities, flag_mask, kernel_index, filter_bank):
    return stream_call(kernel_index, filter_bank, flag_mask[None, :], visibilities)


def solution(mesh):
    placed = (
        P(("group", "tm"), ("bl", "pol"), None, None),
        P(("group", "tm")),
        P(("bl", "pol")),
        P(),
    )
    return jax.shard_map(
        per_device,
        mesh=mesh,
        in_specs=placed,
        out_specs=P("group", ("bl", "pol", "tm"), None, None),
        check_vma=False,
    )
```

```python
import functools

import jax
import jax.numpy as jnp
from jax import lax
from jax.experimental import pallas as pl
from jax.experimental.pallas import tpu as pltpu
from jax.sharding import PartitionSpec as P

TAPS = 257
AVG = 10
HALF = TAPS // 2
SIDE = -(-HALF // AVG)
GROUP = 8
PIECES = 2
LOADS = 3
LEVELS = 32767.0
TINY = 1e-33


def round_up(value, step):
    return -(-value // step) * step


def row_plan(block_rows):
    out_count = block_rows // AVG
    edge, mid = out_count, 2 * SIDE - out_count
    assert 0 < mid < SIDE <= out_count
    edge_rows, mid_rows = round_up(2 * edge, 8), round_up(2 * mid, 8)
    total_rows = 2 * edge_rows + mid_rows
    highest = 2 * (block_rows + HALF + AVG * SIDE)
    lowest = 2 * HALF - 2 * AVG * (SIDE + edge)
    period = round_up(max(highest, 2 * (TAPS + AVG) - lowest), 128)
    return out_count, edge, mid, edge_rows, mid_rows, total_rows, period


def tap_spread(taps):
    width = round_up(2 * (taps + AVG), 128)
    ahead = lax.broadcasted_iota(jnp.int32, (taps, width), 1)
    ahead = ahead - 2 * lax.broadcasted_iota(jnp.int32, (taps, width), 0)
    hit = jnp.logical_and(jnp.logical_and(ahead >= 0, ahead < 2 * AVG), ahead % 2 == 0)
    return jnp.where(hit, 1.0, 0.0).astype(jnp.bfloat16)


def spread_taps(bank_ref, spread):
    filters = bank_ref.shape[1]
    parts = []
    for part in (bank_ref[0], bank_ref[1]):
        for _ in range(3):
            parts.append(part.astype(jnp.bfloat16))
            part = part - parts[-1].astype(jnp.float32)
    total = jnp.dot(jnp.concatenate(parts, axis=0), spread, preferred_element_type=jnp.float32)
    total = [total[filters * k : filters * (k + 1)] for k in range(6)]
    real = (total[0] + total[1] + total[2]) * (1.0 / AVG)
    imag = (total[3] + total[4] + total[5]) * (1.0 / AVG)
    return real - pltpu.roll(imag, 1, 1), imag + pltpu.roll(real, 1, 1)


def flag_spread(block_rows):
    ahead = lax.broadcasted_iota(jnp.int32, (block_rows, 2 * block_rows), 1)
    ahead = ahead - 2 * lax.broadcasted_iota(jnp.int32, (block_rows, 2 * block_rows), 0)
    hit = jnp.logical_and(ahead >= 0, ahead < 2)
    return jnp.where(hit, 1.0, 0.0).astype(jnp.bfloat16)


def spread_flags(flag_ref, spread):
    flags = jnp.broadcast_to(flag_ref[...], (8, flag_ref.shape[1])).astype(jnp.float32)
    return jnp.dot(flags.astype(jnp.bfloat16), spread, preferred_element_type=jnp.float32)


def build_rows(bank_ref, flag_ref, real_ref, imag_ref, good_ref, block_rows, copies):
    period = row_plan(block_rows)[6]
    tap_matrix, flag_matrix = tap_spread(bank_ref.shape[2]), flag_spread(block_rows)
    for copy in copies:
        copy.wait()
    to_real, to_imag = spread_taps(bank_ref, tap_matrix)
    rest = jnp.zeros((to_real.shape[0], period - to_real.shape[1]), jnp.float32)
    real_ref[...] = jnp.concatenate([to_real, rest], axis=1)
    imag_ref[...] = pltpu.roll(jnp.concatenate([to_imag, rest], axis=1), period - AVG, 1)
    good_ref[...] = spread_flags(flag_ref, flag_matrix)


def build_band(real, imag, flags, block_rows):
    out_count, edge, mid, edge_rows, mid_rows, total_rows, period = row_plan(block_rows)
    is_real = lax.broadcasted_iota(jnp.int32, (8, period), 0) % 2 == 0
    tile = jnp.where(
        is_real, jnp.broadcast_to(real, (8, period)), jnp.broadcast_to(imag, (8, period))
    )
    tile = pltpu.roll(tile, 0, 1, stride=AVG, stride_axis=0)
    runs = ((-SIDE, edge, edge_rows), (out_count - SIDE, mid, mid_rows), (SIDE, edge, edge_rows))
    lanes = round_up(2 * block_rows, 128) + 128
    tiles = []
    for first, count, rows in runs:
        for row in range(0, rows, 8):
            start = (2 * HALF - 2 * AVG * first - AVG * row) % period
            aligned = start // 128 * 128
            piece = jnp.concatenate(
                [
                    tile[:, at % period : at % period + 128]
                    for at in range(aligned, aligned + lanes, 128)
                ],
                axis=1,
            )
            piece = pltpu.roll(piece, (aligned - start) % lanes, 1)[:, : 2 * block_rows]
            piece = piece * flags
            if row + 8 > 2 * count:
                at = lax.broadcasted_iota(jnp.int32, piece.shape, 0)
                piece = jnp.where(at < 2 * count - row, piece, 0.0)
            tiles.append(piece)
    band = jnp.concatenate(tiles, axis=0)
    high = band.astype(jnp.bfloat16)
    low = (band - high.astype(jnp.float32)).astype(jnp.bfloat16)
    return jnp.concatenate([high, low], axis=0)


def encode(values, code_ref, step_ref, first=0):
    lane = lax.broadcasted_iota(jnp.int32, (1, 128), 1)
    steps = jnp.zeros((1, 128), jnp.float32)
    for i, value in enumerate(values):
        peak = jnp.max(jnp.max(jnp.abs(value), axis=0, keepdims=True), axis=1, keepdims=True)
        peak = jnp.maximum(peak, TINY)
        steps = jnp.where(lane == i, peak * (1.0 / LEVELS), steps)
        code = jnp.round(value * (LEVELS / peak)).astype(jnp.int32).astype(jnp.int16)
        code_ref[:, first + i] = code.reshape(-1, 2, value.shape[1])
    step_ref[...] = steps


def decode(code):
    rows = code.astype(jnp.int32).astype(jnp.float32)
    return rows.reshape(2 * code.shape[0], code.shape[2])


def stream_kernel(
    index_hbm,
    bank_hbm,
    flag_hbm,
    vis_ref,
    out_ref,
    index_ref,
    bank_ref,
    flag_ref,
    real_ref,
    imag_ref,
    good_ref,
    slab_ref,
    sum_ref,
    edge_ref,
    edge_step_ref,
    mid_ref,
    mid_step_ref,
    in_ref,
    in_edge_step_ref,
    in_mid_step_ref,
    done_ref,
    own_ref,
    small_sem,
    load_sem,
    edge_send,
    edge_step_send,
    mid_send,
    mid_step_send,
    edge_recv,
    edge_step_recv,
    mid_recv,
    mid_step_recv,
    done_send,
    done_recv,
    own_sem,
    lefts_in,
    rights_in,
    *,
    count,
):
    me = lax.axis_index("tm")
    _, block_rows, group, _, channels = slab_ref.shape
    chunks = done_ref.shape[0]
    per_owner = chunks // count
    out_count, edge, mid, edge_rows, mid_rows, total_rows, _ = row_plan(block_rows)
    alone = out_count - SIDE
    mid_at, far_at = edge_rows, edge_rows + mid_rows
    has_left, has_right = me > 0, me < count - 1
    nearer, farther = jnp.minimum(me, count - 1 - me), jnp.maximum(me, count - 1 - me)
    sign = jnp.where(2 * me <= count - 1, 1, -1)

    def chunk_at(step):
        turn, part = step // per_owner, step % per_owner
        late = turn - (farther - nearer)
        flip = jnp.where(late % 2 == 0, sign, -sign)
        owner = jnp.where(
            late < 0, me + sign * (farther - turn), me + flip * (nearer - late // 2)
        )
        return owner, part, owner * per_owner + part

    pieces = load_sem.shape[1]
    share = group // pieces

    def load(step, piece):
        _, _, chunk = chunk_at(step)
        slot = step % LOADS
        return pltpu.make_async_copy(
            vis_ref.at[:, pl.ds(chunk * group + piece * share, share)],
            slab_ref.at[slot, :, pl.ds(piece * share, share)],
            load_sem.at[slot, piece],
        )

    def remote(source, target, send_sem, recv_sem, device):
        return pltpu.make_async_remote_copy(
            src_ref=source,
            dst_ref=target,
            send_sem=send_sem,
            recv_sem=recv_sem,
            device_id={"tm": device},
            device_id_type=pl.DeviceIdType.MESH,
        )

    def slot_of(owner, part, chunk, receiver, rightward):
        second = jnp.logical_and(owner == receiver, jnp.logical_not(rightward))
        return jnp.where(second, chunks + part, chunk)

    def edge_copy(chunk, slot, rightward, device, piece):
        start = jnp.where(rightward, mid, 0)
        lot = pl.ds(piece * share, share)
        return remote(
            edge_ref.at[chunk, :, lot],
            in_ref.at[slot, pl.ds(start, edge), lot],
            edge_send.at[chunk, piece],
            edge_recv.at[slot, piece],
            device,
        )

    def edge_step_copy(chunk, slot, device):
        return remote(
            edge_step_ref.at[chunk],
            in_edge_step_ref.at[slot],
            edge_step_send.at[chunk],
            edge_step_recv.at[slot],
            device,
        )

    def edge_copies(chunk, slot, rightward, device):
        copies = [edge_copy(chunk, slot, rightward, device, piece) for piece in range(pieces)]
        return copies + [edge_step_copy(chunk, slot, device)]

    def mid_copies(chunk, slot, rightward, device):
        start = jnp.where(rightward, 0, edge)
        return (
            remote(
                mid_ref.at[chunk],
                in_ref.at[slot, pl.ds(start, mid)],
                mid_send.at[chunk],
                mid_recv.at[slot],
                device,
            ),
            remote(
                mid_step_ref.at[chunk],
                in_mid_step_ref.at[slot],
                mid_step_send.at[chunk],
                mid_step_recv.at[slot],
                device,
            ),
        )

    def placed(row, rows, part):
        return out_ref.at[pl.ds(row, rows), pl.ds(part * group, group)]

    def full_done(source, chunk, part, rightward, device):
        row = jnp.where(rightward, out_count * (source - 1) + alone, out_count * source + SIDE)
        return remote(
            done_ref.at[chunk],
            placed(row, edge, part),
            done_send.at[chunk],
            done_recv.at[source, part],
            device,
        )

    def short_done(source, chunk, part, rightward, device):
        row = jnp.where(rightward, 0, out_count * source + SIDE)
        start = jnp.where(rightward, SIDE, 0)
        return remote(
            done_ref.at[chunk, pl.ds(start, alone)],
            placed(row, alone, part),
            done_send.at[chunk],
            done_recv.at[source, part],
            device,
        )

    def keep(part, low, rows):
        return pltpu.make_async_copy(
            own_ref.at[part, pl.ds(low, rows)],
            placed(jnp.maximum(out_count * me - SIDE, 0), rows, part),
            own_sem.at[part],
        )

    smalls = [
        pltpu.make_async_copy(source, target, small_sem.at[k])
        for k, (source, target) in enumerate(
            ((bank_hbm, bank_ref), (flag_hbm, flag_ref), (index_hbm, index_ref))
        )
    ]
    for copy in smalls:
        copy.start()
    for piece in range(pieces):
        load(0, piece).start()
    def signal(semaphore, device):
        pl.semaphore_signal(
            semaphore, inc=1, device_id={"tm": device}, device_id_type=pl.DeviceIdType.MESH
        )

    barrier = pltpu.get_barrier_semaphore()

    @pl.when(has_left)
    def _():
        signal(barrier, me - 1)

    @pl.when(has_right)
    def _():
        signal(barrier, me + 1)

    build_rows(bank_ref, flag_ref, real_ref, imag_ref, good_ref, block_rows, smalls)
    for step in range(1, LOADS - 1):
        for piece in range(pieces):
            load(step, piece).start()
    pl.semaphore_wait(barrier, has_left.astype(jnp.int32) + has_right.astype(jnp.int32))

    def flow(owner):
        rightward = owner > me
        upstream = jnp.where(rightward, has_left, has_right)
        return rightward, upstream, jnp.where(rightward, me + 1, me - 1)

    def compute(step, carry):
        @pl.when(step + LOADS - 1 < chunks)
        def _():
            for piece in range(pieces):
                load(step + LOADS - 1, piece).start()

        owner, part, chunk = chunk_at(step)
        slot = step % LOADS
        rightward, upstream, target = flow(owner)
        landing = slot_of(owner, part, chunk, target, rightward)
        for piece in range(pieces):
            load(step, piece).wait()
            lot = range(piece * share, (piece + 1) * share)
            for i in lot:
                which = index_ref[chunk * group + i]
                real, imag = real_ref[pl.ds(which, 1), :], imag_ref[pl.ds(which, 1), :]
                band = build_band(real, imag, good_ref[...], block_rows)
                slab = slab_ref[slot, :, i].reshape(2 * block_rows, channels)
                both = jnp.dot(band, slab, preferred_element_type=jnp.float32)
                sum_ref[chunk, i] = both[:total_rows] + both[total_rows:]

            @pl.when(owner != me)
            def _():
                start = pl.multiple_of(jnp.where(rightward, far_at, 0), 8)
                values = [sum_ref[chunk, i, pl.ds(start, 2 * edge), :] for i in lot]
                encode(values, edge_ref.at[chunk], edge_step_ref.at[chunk, piece], lot[0])
                edge_copy(chunk, landing, rightward, target, piece).start()

        @pl.when(owner != me)
        def _():
            edge_step_copy(chunk, landing, target).start()

        ends = jnp.logical_and(owner != me, jnp.logical_not(upstream))

        @pl.when(ends)
        def _():
            values = [sum_ref[chunk, i, mid_at : mid_at + 2 * mid, :] for i in range(group)]
            encode(values, mid_ref.at[chunk], mid_step_ref.at[chunk])

        turn = step // per_owner
        paired = jnp.logical_or(turn % 2 == 1, turn == count - 2)
        paired = jnp.logical_and(paired, part == per_owner - 1)

        @pl.when(jnp.logical_and(ends, paired))
        def _():
            def start_mid(back, carry):
                owner, part, chunk = chunk_at(back)
                rightward, _, target = flow(owner)
                landing = slot_of(owner, part, chunk, target, rightward)
                for copy in mid_copies(chunk, landing, rightward, target):
                    copy.start()
                return carry

            lax.fori_loop((turn - turn % 2) * per_owner, step + 1, start_mid, 0)

        return carry

    lax.fori_loop(0, chunks, compute, 0)

    @pl.when(has_left)
    def _():
        pl.semaphore_wait(lefts_in, 1)

    @pl.when(has_right)
    def _():
        signal(lefts_in, me + 1)
        pl.semaphore_wait(rights_in, 1)

    @pl.when(has_left)
    def _():
        signal(rights_in, me - 1)

    forward = chunks - per_owner

    def came(slot, start, rows, i):
        return decode(in_ref[slot, pl.ds(start, rows), i])

    def edge_unit(slot, i):
        return in_edge_step_ref[slot, i // share, :, i % share : i % share + 1]

    def pass_mid(step, carry):
        owner, part, chunk = chunk_at(step)
        rightward, upstream, target = flow(owner)
        landing = slot_of(owner, part, chunk, target, rightward)

        @pl.when(upstream)
        def _():
            for copy in edge_copies(chunk, chunk, rightward, target):
                copy.wait_recv()
            start = jnp.where(rightward, edge, 0)
            values = [
                sum_ref[chunk, i, mid_at : mid_at + 2 * mid, :]
                + came(chunk, start, mid, i) * edge_unit(chunk, i)
                for i in range(group)
            ]
            encode(values, mid_ref.at[chunk], mid_step_ref.at[chunk])
            for copy in mid_copies(chunk, landing, rightward, target):
                copy.start()

        return carry

    lax.fori_loop(0, forward, pass_mid, 0)

    def round_off(value, rows):
        return value.astype(jnp.bfloat16).reshape(rows, 2, channels)

    def pass_done(step, carry):
        owner, part, chunk = chunk_at(step)
        rightward, upstream, target = flow(owner)
        near = pl.multiple_of(jnp.where(rightward, 0, far_at), 8)

        @pl.when(upstream)
        def _():
            for copy in mid_copies(chunk, chunk, rightward, target):
                copy.wait_recv()
            start = jnp.where(rightward, 0, mid)
            at = lax.broadcasted_iota(jnp.int32, (2 * edge, channels), 0)
            first = jnp.where(rightward, 0, 2 * (edge - mid))
            of_mid = jnp.logical_and(at >= first, at < first + 2 * mid)
            mids = in_mid_step_ref[chunk]
            for i in range(group):
                unit = jnp.where(of_mid, mids[:, i : i + 1], edge_unit(chunk, i))
                value = sum_ref[chunk, i, pl.ds(near, 2 * edge), :]
                value = value + came(chunk, start, edge, i) * unit
                done_ref[chunk, :, i] = round_off(value, edge)
            full_done(me, chunk, part, rightward, owner).start()

        @pl.when(jnp.logical_not(upstream))
        def _():
            for i in range(group):
                value = sum_ref[chunk, i, pl.ds(near, 2 * edge), :]
                done_ref[chunk, :, i] = round_off(value, edge)
            short_done(me, chunk, part, rightward, owner).start()

        return carry

    lax.fori_loop(0, forward, pass_done, 0)

    def pass_own(part, carry):
        chunk = me * per_owner + part

        def from_side(slot, rightward, near, edge_start, first):
            for copy in edge_copies(chunk, slot, rightward, me):
                copy.wait_recv()
            for copy in mid_copies(chunk, slot, rightward, me):
                copy.wait_recv()
            at = lax.broadcasted_iota(jnp.int32, (2 * edge, channels), 0)
            of_mid = jnp.logical_and(at >= first, at < first + 2 * mid)
            mids = in_mid_step_ref[slot]
            start = edge if rightward else 0
            for i in range(group):
                unit = jnp.where(of_mid, mids[:, i : i + 1], edge_unit(slot, i))
                sum_ref[chunk, i, near : near + 2 * edge, :] += (
                    came(slot, edge_start, edge, i) * unit
                )
                sum_ref[chunk, i, mid_at : mid_at + 2 * mid, :] += (
                    came(slot, start, mid, i) * edge_unit(slot, i)
                )

        @pl.when(has_left)
        def _():
            from_side(chunk, True, 0, 0, 0)

        @pl.when(has_right)
        def _():
            from_side(chunks + part, False, far_at, mid, 2 * (edge - mid))

        for i in range(group):
            for row, rows, start in (
                (0, edge, 0),
                (edge, mid, mid_at),
                (edge + mid, edge, far_at),
            ):
                value = sum_ref[chunk, i, start : start + 2 * rows, :]
                own_ref[part, row : row + rows, i] = round_off(value, rows)

        @pl.when(jnp.logical_and(has_left, has_right))
        def _():
            keep(part, 0, 2 * edge + mid).start()

        @pl.when(jnp.logical_not(has_left))
        def _():
            keep(part, SIDE, out_count + SIDE).start()

        @pl.when(jnp.logical_not(has_right))
        def _():
            keep(part, 0, out_count + SIDE).start()

        return carry

    lax.fori_loop(0, per_owner, pass_own, 0)

    def drain(step, carry):
        owner, part, chunk = chunk_at(step)
        rightward, upstream, target = flow(owner)

        @pl.when(owner != me)
        def _():
            for copy in edge_copies(chunk, chunk, rightward, target):
                copy.wait_send()
            for copy in mid_copies(chunk, chunk, rightward, target):
                copy.wait_send()

            @pl.when(upstream)
            def _():
                full_done(me, chunk, part, rightward, owner).wait_send()

            @pl.when(jnp.logical_not(upstream))
            def _():
                short_done(me, chunk, part, rightward, owner).wait_send()

        @pl.when(owner == me)
        def _():
            @pl.when(jnp.logical_and(has_left, has_right))
            def _():
                keep(part, 0, 2 * edge + mid).wait()

            @pl.when(jnp.logical_not(jnp.logical_and(has_left, has_right)))
            def _():
                keep(part, 0, out_count + SIDE).wait()

        return carry

    lax.fori_loop(0, chunks, drain, 0)

    def collect(turn, carry):
        source = lax.rem(me + 1 + turn, count)
        end = jnp.logical_or(source == 0, source == count - 1)
        for part in range(per_owner):

            @pl.when(end)
            def _():
                short_done(source, 0, part, source < me, source).wait_recv()

            @pl.when(jnp.logical_not(end))
            def _():
                full_done(source, 0, part, source < me, source).wait_recv()

        return carry

    lax.fori_loop(0, count - 1, collect, 0)


def stream_call(kernel_index, filter_bank, flags, visibilities):
    block_rows, bases, _, channels = visibilities.shape
    count = lax.axis_size("tm")
    out_count, edge, mid, _, _, total_rows, period = row_plan(block_rows)
    filters = filter_bank.shape[1]
    owned = bases // count
    group = GROUP
    while owned % group:
        group //= 2
    chunks, parts, pieces = bases // group, owned // group, min(PIECES, group)
    slots = chunks + parts
    small = [
        pltpu.with_memory_space_constraint(operand, pltpu.HBM)
        for operand in (kernel_index, filter_bank, flags)
    ]
    sent, landed = pltpu.SemaphoreType.DMA((chunks,)), pltpu.SemaphoreType.DMA((slots,))
    return pl.pallas_call(
        functools.partial(stream_kernel, count=count),
        in_specs=[
            pl.BlockSpec(memory_space=pltpu.HBM),
            pl.BlockSpec(memory_space=pltpu.HBM),
            pl.BlockSpec(memory_space=pltpu.HBM),
            pl.BlockSpec(memory_space=pl.ANY),
        ],
        out_specs=pl.BlockSpec(memory_space=pl.ANY),
        out_shape=jax.ShapeDtypeStruct((count * out_count, owned, 2, channels), jnp.bfloat16),
        scratch_shapes=[
            pltpu.SMEM(kernel_index.shape, jnp.int32),
            pltpu.VMEM(filter_bank.shape, jnp.float32),
            pltpu.VMEM(flags.shape, jnp.int32),
            pltpu.VMEM((filters, period), jnp.float32),
            pltpu.VMEM((filters, period), jnp.float32),
            pltpu.VMEM((8, 2 * block_rows), jnp.float32),
            pltpu.VMEM((LOADS, block_rows, group, 2, channels), jnp.bfloat16),
            pltpu.VMEM((chunks, group, total_rows, channels), jnp.float32),
            pltpu.VMEM((chunks, edge, group, 2, channels), jnp.int16),
            pltpu.VMEM((chunks, pieces, 1, 128), jnp.float32),
            pltpu.VMEM((chunks, mid, group, 2, channels), jnp.int16),
            pltpu.VMEM((chunks, 1, 128), jnp.float32),
            pltpu.VMEM((slots, edge + mid, group, 2, channels), jnp.int16),
            pltpu.VMEM((slots, pieces, 1, 128), jnp.float32),
            pltpu.VMEM((slots, 1, 128), jnp.float32),
            pltpu.VMEM((chunks, edge, group, 2, channels), jnp.bfloat16),
            pltpu.VMEM((parts, 2 * edge + mid, group, 2, channels), jnp.bfloat16),
            pltpu.SemaphoreType.DMA((3,)),
            pltpu.SemaphoreType.DMA((LOADS, pieces)),
            pltpu.SemaphoreType.DMA((chunks, pieces)),
            sent,
            sent,
            sent,
            pltpu.SemaphoreType.DMA((slots, pieces)),
            landed,
            landed,
            landed,
            sent,
            pltpu.SemaphoreType.DMA((count, parts)),
            pltpu.SemaphoreType.DMA((parts,)),
            pltpu.SemaphoreType.REGULAR,
            pltpu.SemaphoreType.REGULAR,
        ],
        compiler_params=pltpu.CompilerParams(
            collective_id=0, has_side_effects=True, vmem_limit_bytes=40 * 1024 * 1024
        ),
    )(*small, visibilities)


def per_device(visibilities, flag_mask, kernel_index, filter_bank):
    return stream_call(kernel_index, filter_bank, flag_mask[None, :], visibilities)


def solution(mesh):
    placed = (
        P(("group", "tm"), ("bl", "pol"), None, None),
        P(("group", "tm")),
        P(("bl", "pol")),
        P(),
    )
    return jax.shard_map(
        per_device,
        mesh=mesh,
        in_specs=placed,
        out_specs=P("group", ("bl", "pol", "tm"), None, None),
        check_vma=False,
    )
```

```python
import functools

import jax
import jax.numpy as jnp
from jax import lax
from jax.experimental import pallas as pl
from jax.experimental.pallas import tpu as pltpu
from jax.sharding import PartitionSpec as P

TAPS = 257
AVG = 10
HALF = TAPS // 2
SIDE = -(-HALF // AVG)
GROUP = 8
LOADS = 3
LEVELS = 32767.0
TINY = 1e-33


def round_up(value, step):
    return -(-value // step) * step


def row_plan(block_rows):
    out_count = block_rows // AVG
    edge, mid = out_count, 2 * SIDE - out_count
    assert 0 < mid < SIDE <= out_count
    edge_rows, mid_rows = round_up(2 * edge, 8), round_up(2 * mid, 8)
    total_rows = 2 * edge_rows + mid_rows
    highest = 2 * (block_rows + HALF + AVG * SIDE)
    lowest = 2 * HALF - 2 * AVG * (SIDE + edge)
    period = round_up(max(highest, 2 * (TAPS + AVG) - lowest), 128)
    return out_count, edge, mid, edge_rows, mid_rows, total_rows, period


def tap_spread(taps):
    width = round_up(2 * (taps + AVG), 128)
    ahead = lax.broadcasted_iota(jnp.int32, (taps, width), 1)
    ahead = ahead - 2 * lax.broadcasted_iota(jnp.int32, (taps, width), 0)
    hit = jnp.logical_and(jnp.logical_and(ahead >= 0, ahead < 2 * AVG), ahead % 2 == 0)
    return jnp.where(hit, 1.0, 0.0).astype(jnp.bfloat16)


def spread_taps(bank_ref, spread):
    filters = bank_ref.shape[1]
    parts = []
    for part in (bank_ref[0], bank_ref[1]):
        for _ in range(3):
            parts.append(part.astype(jnp.bfloat16))
            part = part - parts[-1].astype(jnp.float32)
    total = jnp.dot(jnp.concatenate(parts, axis=0), spread, preferred_element_type=jnp.float32)
    total = [total[filters * k : filters * (k + 1)] for k in range(6)]
    real = (total[0] + total[1] + total[2]) * (1.0 / AVG)
    imag = (total[3] + total[4] + total[5]) * (1.0 / AVG)
    return real - pltpu.roll(imag, 1, 1), imag + pltpu.roll(real, 1, 1)


def flag_spread(block_rows):
    ahead = lax.broadcasted_iota(jnp.int32, (block_rows, 2 * block_rows), 1)
    ahead = ahead - 2 * lax.broadcasted_iota(jnp.int32, (block_rows, 2 * block_rows), 0)
    hit = jnp.logical_and(ahead >= 0, ahead < 2)
    return jnp.where(hit, 1.0, 0.0).astype(jnp.bfloat16)


def spread_flags(flag_ref, spread):
    flags = jnp.broadcast_to(flag_ref[...], (8, flag_ref.shape[1])).astype(jnp.float32)
    return jnp.dot(flags.astype(jnp.bfloat16), spread, preferred_element_type=jnp.float32)


def build_rows(bank_ref, flag_ref, real_ref, imag_ref, good_ref, block_rows, copies):
    period = row_plan(block_rows)[6]
    tap_matrix, flag_matrix = tap_spread(bank_ref.shape[2]), flag_spread(block_rows)
    for copy in copies:
        copy.wait()
    to_real, to_imag = spread_taps(bank_ref, tap_matrix)
    rest = jnp.zeros((to_real.shape[0], period - to_real.shape[1]), jnp.float32)
    real_ref[...] = jnp.concatenate([to_real, rest], axis=1)
    imag_ref[...] = pltpu.roll(jnp.concatenate([to_imag, rest], axis=1), period - AVG, 1)
    good_ref[...] = spread_flags(flag_ref, flag_matrix)


def runs_of(block_rows):
    out_count, edge, mid, edge_rows, mid_rows, _, _ = row_plan(block_rows)
    return (-SIDE, edge, edge_rows), (out_count - SIDE, mid, mid_rows), (SIDE, edge, edge_rows)


def build_band(real, imag, flags, block_rows, runs):
    period = row_plan(block_rows)[6]
    is_real = lax.broadcasted_iota(jnp.int32, (8, period), 0) % 2 == 0
    tile = jnp.where(
        is_real, jnp.broadcast_to(real, (8, period)), jnp.broadcast_to(imag, (8, period))
    )
    tile = pltpu.roll(tile, 0, 1, stride=AVG, stride_axis=0)
    lanes = round_up(2 * block_rows, 128) + 128
    tiles = []
    for first, count, rows in runs:
        for row in range(0, rows, 8):
            start = (2 * HALF - 2 * AVG * first - AVG * row) % period
            aligned = start // 128 * 128
            piece = jnp.concatenate(
                [
                    tile[:, at % period : at % period + 128]
                    for at in range(aligned, aligned + lanes, 128)
                ],
                axis=1,
            )
            piece = pltpu.roll(piece, (aligned - start) % lanes, 1)[:, : 2 * block_rows]
            piece = piece * flags
            if row + 8 > 2 * count:
                at = lax.broadcasted_iota(jnp.int32, piece.shape, 0)
                piece = jnp.where(at < 2 * count - row, piece, 0.0)
            tiles.append(piece)
    band = jnp.concatenate(tiles, axis=0)
    high = band.astype(jnp.bfloat16)
    low = (band - high.astype(jnp.float32)).astype(jnp.bfloat16)
    return jnp.concatenate([high, low], axis=0)


def lots_of(group):
    first = max(3 * group // 8, 1)
    return [(0, first), (first, group - first)] if group > first else [(0, group)]


def encode(values, code_ref, step_ref, first=0):
    lane = lax.broadcasted_iota(jnp.int32, (1, 128), 1)
    steps = jnp.zeros((1, 128), jnp.float32)
    for i, value in enumerate(values):
        peak = jnp.max(jnp.max(jnp.abs(value), axis=0, keepdims=True), axis=1, keepdims=True)
        peak = jnp.maximum(peak, TINY)
        steps = jnp.where(lane == i, peak * (1.0 / LEVELS), steps)
        code = jnp.round(value * (LEVELS / peak)).astype(jnp.int32).astype(jnp.int16)
        code_ref[:, first + i] = code.reshape(-1, 2, value.shape[1])
    step_ref[...] = steps


def decode(code):
    rows = code.astype(jnp.int32).astype(jnp.float32)
    return rows.reshape(2 * code.shape[0], code.shape[2])


def stream_kernel(
    index_hbm,
    bank_hbm,
    flag_hbm,
    vis_ref,
    out_ref,
    index_ref,
    bank_ref,
    flag_ref,
    real_ref,
    imag_ref,
    good_ref,
    band_ref,
    slab_ref,
    sum_ref,
    edge_ref,
    edge_step_ref,
    mid_ref,
    mid_step_ref,
    in_ref,
    in_edge_step_ref,
    in_mid_step_ref,
    done_ref,
    own_ref,
    small_sem,
    load_sem,
    edge_send,
    edge_step_send,
    mid_send,
    mid_step_send,
    edge_recv,
    edge_step_recv,
    mid_recv,
    mid_step_recv,
    done_send,
    done_recv,
    own_sem,
    lefts_in,
    rights_in,
    *,
    count,
):
    me = lax.axis_index("tm")
    loads, block_rows, group, _, channels = slab_ref.shape
    chunks = done_ref.shape[0]
    per_owner = chunks // count
    out_count, edge, mid, edge_rows, mid_rows, total_rows, _ = row_plan(block_rows)
    alone = out_count - SIDE
    mid_at, far_at = edge_rows, edge_rows + mid_rows
    has_left, has_right = me > 0, me < count - 1
    nearer, farther = jnp.minimum(me, count - 1 - me), jnp.maximum(me, count - 1 - me)
    sign = jnp.where(2 * me <= count - 1, 1, -1)

    def chunk_at(step):
        turn, part = step // per_owner, step % per_owner
        late = turn - (farther - nearer)
        flip = jnp.where(late % 2 == 0, sign, -sign)
        owner = jnp.where(
            late < 0, me + sign * (farther - turn), me + flip * (nearer - late // 2)
        )
        return owner, part, owner * per_owner + part

    lots = lots_of(group)
    pieces = range(len(lots))

    def load(step, piece):
        _, _, chunk = chunk_at(step)
        slot = step % loads
        start, size = lots[piece]
        return pltpu.make_async_copy(
            vis_ref.at[:, pl.ds(chunk * group + start, size)],
            slab_ref.at[slot, :, pl.ds(start, size)],
            load_sem.at[slot, piece],
        )

    def remote(source, target, send_sem, recv_sem, device):
        return pltpu.make_async_remote_copy(
            src_ref=source,
            dst_ref=target,
            send_sem=send_sem,
            recv_sem=recv_sem,
            device_id={"tm": device},
            device_id_type=pl.DeviceIdType.MESH,
        )

    def slot_of(owner, part, chunk, receiver, rightward):
        second = jnp.logical_and(owner == receiver, jnp.logical_not(rightward))
        return jnp.where(second, chunks + part, chunk)

    def edge_copy(chunk, slot, rightward, device, piece):
        start = jnp.where(rightward, mid, 0)
        lot = pl.ds(*lots[piece])
        return remote(
            edge_ref.at[chunk, :, lot],
            in_ref.at[slot, pl.ds(start, edge), lot],
            edge_send.at[chunk, piece],
            edge_recv.at[slot, piece],
            device,
        )

    def edge_step_copy(chunk, slot, device):
        return remote(
            edge_step_ref.at[chunk],
            in_edge_step_ref.at[slot],
            edge_step_send.at[chunk],
            edge_step_recv.at[slot],
            device,
        )

    def edge_copies(chunk, slot, rightward, device):
        copies = [edge_copy(chunk, slot, rightward, device, piece) for piece in pieces]
        return copies + [edge_step_copy(chunk, slot, device)]

    def mid_copies(chunk, slot, rightward, device):
        start = jnp.where(rightward, 0, edge)
        return (
            remote(
                mid_ref.at[chunk],
                in_ref.at[slot, pl.ds(start, mid)],
                mid_send.at[chunk],
                mid_recv.at[slot],
                device,
            ),
            remote(
                mid_step_ref.at[chunk],
                in_mid_step_ref.at[slot],
                mid_step_send.at[chunk],
                mid_step_recv.at[slot],
                device,
            ),
        )

    def placed(row, rows, part):
        return out_ref.at[pl.ds(row, rows), pl.ds(part * group, group)]

    def full_done(source, chunk, part, rightward, device):
        row = jnp.where(rightward, out_count * (source - 1) + alone, out_count * source + SIDE)
        return remote(
            done_ref.at[chunk],
            placed(row, edge, part),
            done_send.at[chunk],
            done_recv.at[source, part],
            device,
        )

    def short_done(source, chunk, part, rightward, device):
        row = jnp.where(rightward, 0, out_count * source + SIDE)
        start = jnp.where(rightward, SIDE, 0)
        return remote(
            done_ref.at[chunk, pl.ds(start, alone)],
            placed(row, alone, part),
            done_send.at[chunk],
            done_recv.at[source, part],
            device,
        )

    def keep(part, low, rows):
        return pltpu.make_async_copy(
            own_ref.at[part, pl.ds(low, rows)],
            placed(jnp.maximum(out_count * me - SIDE, 0), rows, part),
            own_sem.at[part],
        )

    smalls = [
        pltpu.make_async_copy(source, target, small_sem.at[k])
        for k, (source, target) in enumerate(
            ((bank_hbm, bank_ref), (flag_hbm, flag_ref), (index_hbm, index_ref))
        )
    ]
    for copy in smalls:
        copy.start()
    for piece in pieces:
        load(0, piece).start()
    def signal(semaphore, device):
        pl.semaphore_signal(
            semaphore, inc=1, device_id={"tm": device}, device_id_type=pl.DeviceIdType.MESH
        )

    barrier = pltpu.get_barrier_semaphore()

    @pl.when(has_left)
    def _():
        signal(barrier, me - 1)

    @pl.when(has_right)
    def _():
        signal(barrier, me + 1)

    build_rows(bank_ref, flag_ref, real_ref, imag_ref, good_ref, block_rows, smalls)
    for step in range(1, loads - 1):
        for piece in pieces:
            load(step, piece).start()
    pl.semaphore_wait(barrier, has_left.astype(jnp.int32) + has_right.astype(jnp.int32))

    def flow(owner):
        rightward = owner > me
        upstream = jnp.where(rightward, has_left, has_right)
        return rightward, upstream, jnp.where(rightward, me + 1, me - 1)

    def baseline(chunk, slot, i, band):
        slab = slab_ref[slot, :, i].reshape(2 * block_rows, channels)
        both = jnp.dot(band, slab, preferred_element_type=jnp.float32)
        sum_ref[chunk, i] = both[:total_rows] + both[total_rows:]

    def rows_of(which):
        return real_ref[pl.ds(which, 1), :], imag_ref[pl.ds(which, 1), :]

    def send_edges(owner, part, chunk, piece):
        rightward, _, target = flow(owner)
        landing = slot_of(owner, part, chunk, target, rightward)
        near = pl.multiple_of(jnp.where(rightward, far_at, 0), 8)
        start, size = lots[piece]
        values = [
            sum_ref[chunk, i, pl.ds(near, 2 * edge), :] for i in range(start, start + size)
        ]
        encode(values, edge_ref.at[chunk], edge_step_ref.at[chunk, piece], start)
        edge_copy(chunk, landing, rightward, target, piece).start()
        if piece == len(lots) - 1:
            edge_step_copy(chunk, landing, target).start()

    def prefetch(step):
        @pl.when(step + loads - 1 < chunks)
        def _():
            for piece in pieces:
                load(step + loads - 1, piece).start()

    def compute_ends(step, carry):
        owner, part, chunk = chunk_at(step)
        _, upstream, _ = flow(owner)

        ends = jnp.logical_and(owner != me, jnp.logical_not(upstream))

        @pl.when(ends)
        def _():
            values = [sum_ref[chunk, i, mid_at : mid_at + 2 * mid, :] for i in range(group)]
            encode(values, mid_ref.at[chunk], mid_step_ref.at[chunk])

        turn = step // per_owner
        paired = jnp.logical_or(turn % 2 == 1, turn == count - 2)
        paired = jnp.logical_and(paired, part == per_owner - 1)

        @pl.when(jnp.logical_and(ends, paired))
        def _():
            def start_mid(back, carry):
                owner, part, chunk = chunk_at(back)
                rightward, _, target = flow(owner)
                landing = slot_of(owner, part, chunk, target, rightward)
                for copy in mid_copies(chunk, landing, rightward, target):
                    copy.start()
                return carry

            lax.fori_loop((turn - turn % 2) * per_owner, step + 1, start_mid, 0)

        return carry

    runs = runs_of(block_rows)

    def first_edges(run, near, rows):
        def one_chunk(step, carry):
            owner, part, chunk = chunk_at(step)
            for piece in pieces:
                load(step, piece).wait()
                for i in range(lots[piece][0], sum(lots[piece])):
                    real, imag = rows_of(index_ref[chunk * group + i])
                    band = build_band(real, imag, good_ref[...], block_rows, (run,))
                    slab = slab_ref[step % loads, :, i].reshape(2 * block_rows, channels)
                    both = jnp.dot(band, slab, preferred_element_type=jnp.float32)
                    sum_ref[chunk, i, near : near + rows, :] = both[:rows] + both[rows:]
                send_edges(owner, part, chunk, piece)
            return carry

        lax.fori_loop(0, per_owner, one_chunk, 0)

    right_first = chunk_at(0)[0] > me

    @pl.when(right_first)
    def _():
        first_edges(runs[2], far_at, edge_rows)

    @pl.when(jnp.logical_not(right_first))
    def _():
        first_edges(runs[0], 0, edge_rows)

    def one_band(f, carry):
        band_ref[f] = build_band(*rows_of(f), good_ref[...], block_rows, runs)
        return carry

    lax.fori_loop(0, real_ref.shape[0], one_band, 0, unroll=2)

    def compute(step, carry):
        prefetch(step)
        owner, part, chunk = chunk_at(step)
        slot = step % loads

        @pl.when(step >= per_owner)
        def _():
            for piece in pieces:
                load(step, piece).wait()

        for i in range(group):
            baseline(chunk, slot, i, band_ref[index_ref[chunk * group + i]])

        @pl.when(jnp.logical_and(step >= per_owner, owner != me))
        def _():
            for piece in pieces:
                send_edges(owner, part, chunk, piece)

        return carry

    lax.fori_loop(0, chunks, lambda step, carry: compute_ends(step, compute(step, carry)), 0)

    @pl.when(has_left)
    def _():
        pl.semaphore_wait(lefts_in, 1)

    @pl.when(has_right)
    def _():
        signal(lefts_in, me + 1)
        pl.semaphore_wait(rights_in, 1)

    @pl.when(has_left)
    def _():
        signal(rights_in, me - 1)

    forward = chunks - per_owner

    def came(slot, start, rows, i):
        return decode(in_ref[slot, pl.ds(start, rows), i])

    def edge_unit(slot, i):
        piece = [i >= start for start, _ in lots].count(True) - 1
        lane = i - lots[piece][0]
        return in_edge_step_ref[slot, piece, :, lane : lane + 1]

    def pass_mid(step, carry):
        owner, part, chunk = chunk_at(step)
        rightward, upstream, target = flow(owner)
        landing = slot_of(owner, part, chunk, target, rightward)

        @pl.when(upstream)
        def _():
            for copy in edge_copies(chunk, chunk, rightward, target):
                copy.wait_recv()
            start = jnp.where(rightward, edge, 0)
            values = [
                sum_ref[chunk, i, mid_at : mid_at + 2 * mid, :]
                + came(chunk, start, mid, i) * edge_unit(chunk, i)
                for i in range(group)
            ]
            encode(values, mid_ref.at[chunk], mid_step_ref.at[chunk])
            for copy in mid_copies(chunk, landing, rightward, target):
                copy.start()

        return carry

    lax.fori_loop(0, forward, pass_mid, 0)

    def round_off(value, rows):
        return value.astype(jnp.bfloat16).reshape(rows, 2, channels)

    def pass_done(step, carry):
        owner, part, chunk = chunk_at(step)
        rightward, upstream, target = flow(owner)
        near = pl.multiple_of(jnp.where(rightward, 0, far_at), 8)

        @pl.when(upstream)
        def _():
            for copy in mid_copies(chunk, chunk, rightward, target):
                copy.wait_recv()
            start = jnp.where(rightward, 0, mid)
            at = lax.broadcasted_iota(jnp.int32, (2 * edge, channels), 0)
            first = jnp.where(rightward, 0, 2 * (edge - mid))
            of_mid = jnp.logical_and(at >= first, at < first + 2 * mid)
            mids = in_mid_step_ref[chunk]
            for i in range(group):
                unit = jnp.where(of_mid, mids[:, i : i + 1], edge_unit(chunk, i))
                value = sum_ref[chunk, i, pl.ds(near, 2 * edge), :]
                value = value + came(chunk, start, edge, i) * unit
                done_ref[chunk, :, i] = round_off(value, edge)
            full_done(me, chunk, part, rightward, owner).start()

        @pl.when(jnp.logical_not(upstream))
        def _():
            for i in range(group):
                value = sum_ref[chunk, i, pl.ds(near, 2 * edge), :]
                done_ref[chunk, :, i] = round_off(value, edge)
            short_done(me, chunk, part, rightward, owner).start()

        return carry

    lax.fori_loop(0, forward, pass_done, 0)

    def pass_own(part, carry):
        chunk = me * per_owner + part

        def from_side(slot, rightward, near, edge_start, first):
            for copy in edge_copies(chunk, slot, rightward, me):
                copy.wait_recv()
            for copy in mid_copies(chunk, slot, rightward, me):
                copy.wait_recv()
            at = lax.broadcasted_iota(jnp.int32, (2 * edge, channels), 0)
            of_mid = jnp.logical_and(at >= first, at < first + 2 * mid)
            mids = in_mid_step_ref[slot]
            start = edge if rightward else 0
            for i in range(group):
                unit = jnp.where(of_mid, mids[:, i : i + 1], edge_unit(slot, i))
                sum_ref[chunk, i, near : near + 2 * edge, :] += (
                    came(slot, edge_start, edge, i) * unit
                )
                sum_ref[chunk, i, mid_at : mid_at + 2 * mid, :] += (
                    came(slot, start, mid, i) * edge_unit(slot, i)
                )

        @pl.when(has_left)
        def _():
            from_side(chunk, True, 0, 0, 0)

        @pl.when(has_right)
        def _():
            from_side(chunks + part, False, far_at, mid, 2 * (edge - mid))

        for i in range(group):
            for row, rows, start in (
                (0, edge, 0),
                (edge, mid, mid_at),
                (edge + mid, edge, far_at),
            ):
                value = sum_ref[chunk, i, start : start + 2 * rows, :]
                own_ref[part, row : row + rows, i] = round_off(value, rows)

        @pl.when(jnp.logical_and(has_left, has_right))
        def _():
            keep(part, 0, 2 * edge + mid).start()

        @pl.when(jnp.logical_not(has_left))
        def _():
            keep(part, SIDE, out_count + SIDE).start()

        @pl.when(jnp.logical_not(has_right))
        def _():
            keep(part, 0, out_count + SIDE).start()

        return carry

    lax.fori_loop(0, per_owner, pass_own, 0)

    def drain(step, carry):
        owner, part, chunk = chunk_at(step)
        rightward, upstream, target = flow(owner)

        @pl.when(owner != me)
        def _():
            for copy in edge_copies(chunk, chunk, rightward, target):
                copy.wait_send()
            for copy in mid_copies(chunk, chunk, rightward, target):
                copy.wait_send()

            @pl.when(upstream)
            def _():
                full_done(me, chunk, part, rightward, owner).wait_send()

            @pl.when(jnp.logical_not(upstream))
            def _():
                short_done(me, chunk, part, rightward, owner).wait_send()

        @pl.when(owner == me)
        def _():
            @pl.when(jnp.logical_and(has_left, has_right))
            def _():
                keep(part, 0, 2 * edge + mid).wait()

            @pl.when(jnp.logical_not(jnp.logical_and(has_left, has_right)))
            def _():
                keep(part, 0, out_count + SIDE).wait()

        return carry

    lax.fori_loop(0, chunks, drain, 0)

    def collect(turn, carry):
        source = lax.rem(me + 1 + turn, count)
        end = jnp.logical_or(source == 0, source == count - 1)
        for part in range(per_owner):

            @pl.when(end)
            def _():
                short_done(source, 0, part, source < me, source).wait_recv()

            @pl.when(jnp.logical_not(end))
            def _():
                full_done(source, 0, part, source < me, source).wait_recv()

        return carry

    lax.fori_loop(0, count - 1, collect, 0)


def stream_call(kernel_index, filter_bank, flags, visibilities):
    block_rows, bases, _, channels = visibilities.shape
    count = lax.axis_size("tm")
    out_count, edge, mid, _, _, total_rows, period = row_plan(block_rows)
    filters = filter_bank.shape[1]
    owned = bases // count
    group = GROUP
    while owned % group:
        group //= 2
    chunks, parts, pieces = bases // group, owned // group, len(lots_of(group))
    slots = chunks + parts
    loads = max(LOADS, parts + 1)
    small = [
        pltpu.with_memory_space_constraint(operand, pltpu.HBM)
        for operand in (kernel_index, filter_bank, flags)
    ]
    sent, landed = pltpu.SemaphoreType.DMA((chunks,)), pltpu.SemaphoreType.DMA((slots,))
    return pl.pallas_call(
        functools.partial(stream_kernel, count=count),
        in_specs=[
            pl.BlockSpec(memory_space=pltpu.HBM),
            pl.BlockSpec(memory_space=pltpu.HBM),
            pl.BlockSpec(memory_space=pltpu.HBM),
            pl.BlockSpec(memory_space=pl.ANY),
        ],
        out_specs=pl.BlockSpec(memory_space=pl.ANY),
        out_shape=jax.ShapeDtypeStruct((count * out_count, owned, 2, channels), jnp.bfloat16),
        scratch_shapes=[
            pltpu.SMEM(kernel_index.shape, jnp.int32),
            pltpu.VMEM(filter_bank.shape, jnp.float32),
            pltpu.VMEM(flags.shape, jnp.int32),
            pltpu.VMEM((filters, period), jnp.float32),
            pltpu.VMEM((filters, period), jnp.float32),
            pltpu.VMEM((8, 2 * block_rows), jnp.float32),
            pltpu.VMEM((filters, 2 * total_rows, 2 * block_rows), jnp.bfloat16),
            pltpu.VMEM((loads, block_rows, group, 2, channels), jnp.bfloat16),
            pltpu.VMEM((chunks, group, total_rows, channels), jnp.float32),
            pltpu.VMEM((chunks, edge, group, 2, channels), jnp.int16),
            pltpu.VMEM((chunks, pieces, 1, 128), jnp.float32),
            pltpu.VMEM((chunks, mid, group, 2, channels), jnp.int16),
            pltpu.VMEM((chunks, 1, 128), jnp.float32),
            pltpu.VMEM((slots, edge + mid, group, 2, channels), jnp.int16),
            pltpu.VMEM((slots, pieces, 1, 128), jnp.float32),
            pltpu.VMEM((slots, 1, 128), jnp.float32),
            pltpu.VMEM((chunks, edge, group, 2, channels), jnp.bfloat16),
            pltpu.VMEM((parts, 2 * edge + mid, group, 2, channels), jnp.bfloat16),
            pltpu.SemaphoreType.DMA((3,)),
            pltpu.SemaphoreType.DMA((loads, pieces)),
            pltpu.SemaphoreType.DMA((chunks, pieces)),
            sent,
            sent,
            sent,
            pltpu.SemaphoreType.DMA((slots, pieces)),
            landed,
            landed,
            landed,
            sent,
            pltpu.SemaphoreType.DMA((count, parts)),
            pltpu.SemaphoreType.DMA((parts,)),
            pltpu.SemaphoreType.REGULAR,
            pltpu.SemaphoreType.REGULAR,
        ],
        compiler_params=pltpu.CompilerParams(
            collective_id=0, has_side_effects=True, vmem_limit_bytes=40 * 1024 * 1024
        ),
    )(*small, visibilities)


def per_device(visibilities, flag_mask, kernel_index, filter_bank):
    return stream_call(kernel_index, filter_bank, flag_mask[None, :], visibilities)


def solution(mesh):
    placed = (
        P(("group", "tm"), ("bl", "pol"), None, None),
        P(("group", "tm")),
        P(("bl", "pol")),
        P(),
    )
    return jax.shard_map(
        per_device,
        mesh=mesh,
        in_specs=placed,
        out_specs=P("group", ("bl", "pol", "tm"), None, None),
        check_vma=False,
    )
```

```python
import functools

import jax
import jax.numpy as jnp
from jax import lax
from jax.experimental import pallas as pl
from jax.experimental.pallas import tpu as pltpu
from jax.sharding import PartitionSpec as P

TAPS = 257
AVG = 10
HALF = TAPS // 2
SIDE = -(-HALF // AVG)
GROUP = 8
LOADS = 3
LEVELS = 32767.0
TINY = 1e-33


def round_up(value, step):
    return -(-value // step) * step


def row_plan(block_rows):
    out_count = block_rows // AVG
    edge, mid = out_count, 2 * SIDE - out_count
    assert 0 < mid < SIDE <= out_count
    edge_rows, mid_rows = round_up(2 * edge, 8), round_up(2 * mid, 8)
    total_rows = 2 * edge_rows + mid_rows
    highest = 2 * (block_rows + HALF + AVG * SIDE)
    lowest = 2 * HALF - 2 * AVG * (SIDE + edge)
    period = round_up(max(highest, 2 * (TAPS + AVG) - lowest), 128)
    return out_count, edge, mid, edge_rows, mid_rows, total_rows, period


def tap_spread(taps):
    width = round_up(2 * (taps + AVG), 128)
    ahead = lax.broadcasted_iota(jnp.int32, (taps, width), 1)
    ahead = ahead - 2 * lax.broadcasted_iota(jnp.int32, (taps, width), 0)
    hit = jnp.logical_and(jnp.logical_and(ahead >= 0, ahead < 2 * AVG), ahead % 2 == 0)
    return jnp.where(hit, 1.0, 0.0).astype(jnp.bfloat16)


def spread_taps(bank_ref, spread):
    filters = bank_ref.shape[1]
    parts = []
    for part in (bank_ref[0], bank_ref[1]):
        for _ in range(3):
            parts.append(part.astype(jnp.bfloat16))
            part = part - parts[-1].astype(jnp.float32)
    total = jnp.dot(jnp.concatenate(parts, axis=0), spread, preferred_element_type=jnp.float32)
    total = [total[filters * k : filters * (k + 1)] for k in range(6)]
    real = (total[0] + total[1] + total[2]) * (1.0 / AVG)
    imag = (total[3] + total[4] + total[5]) * (1.0 / AVG)
    return real - pltpu.roll(imag, 1, 1), imag + pltpu.roll(real, 1, 1)


def flag_spread(block_rows):
    ahead = lax.broadcasted_iota(jnp.int32, (block_rows, 2 * block_rows), 1)
    ahead = ahead - 2 * lax.broadcasted_iota(jnp.int32, (block_rows, 2 * block_rows), 0)
    hit = jnp.logical_and(ahead >= 0, ahead < 2)
    return jnp.where(hit, 1.0, 0.0).astype(jnp.bfloat16)


def spread_flags(flag_ref, spread):
    flags = jnp.broadcast_to(flag_ref[...], (8, flag_ref.shape[1])).astype(jnp.float32)
    return jnp.dot(flags.astype(jnp.bfloat16), spread, preferred_element_type=jnp.float32)


def build_rows(bank_ref, flag_ref, real_ref, imag_ref, good_ref, block_rows, copies):
    period = row_plan(block_rows)[6]
    tap_matrix, flag_matrix = tap_spread(bank_ref.shape[2]), flag_spread(block_rows)
    for copy in copies:
        copy.wait()
    to_real, to_imag = spread_taps(bank_ref, tap_matrix)
    rest = jnp.zeros((to_real.shape[0], period - to_real.shape[1]), jnp.float32)
    real_ref[...] = jnp.concatenate([to_real, rest], axis=1)
    imag_ref[...] = pltpu.roll(jnp.concatenate([to_imag, rest], axis=1), period - AVG, 1)
    good_ref[...] = spread_flags(flag_ref, flag_matrix)


def runs_of(block_rows):
    out_count, edge, mid, edge_rows, mid_rows, _, _ = row_plan(block_rows)
    return (-SIDE, edge, edge_rows), (out_count - SIDE, mid, mid_rows), (SIDE, edge, edge_rows)


def build_band(real, imag, flags, block_rows, runs):
    period = row_plan(block_rows)[6]
    is_real = lax.broadcasted_iota(jnp.int32, (8, period), 0) % 2 == 0
    tile = jnp.where(
        is_real, jnp.broadcast_to(real, (8, period)), jnp.broadcast_to(imag, (8, period))
    )
    tile = pltpu.roll(tile, 0, 1, stride=AVG, stride_axis=0)
    lanes = round_up(2 * block_rows, 128) + 128
    tiles = []
    for first, count, rows in runs:
        for row in range(0, rows, 8):
            start = (2 * HALF - 2 * AVG * first - AVG * row) % period
            aligned = start // 128 * 128
            piece = jnp.concatenate(
                [
                    tile[:, at % period : at % period + 128]
                    for at in range(aligned, aligned + lanes, 128)
                ],
                axis=1,
            )
            piece = pltpu.roll(piece, (aligned - start) % lanes, 1)[:, : 2 * block_rows]
            piece = piece * flags
            if row + 8 > 2 * count:
                at = lax.broadcasted_iota(jnp.int32, piece.shape, 0)
                piece = jnp.where(at < 2 * count - row, piece, 0.0)
            tiles.append(piece)
    band = jnp.concatenate(tiles, axis=0)
    high = band.astype(jnp.bfloat16)
    low = (band - high.astype(jnp.float32)).astype(jnp.bfloat16)
    return jnp.concatenate([high, low], axis=0)


def lots_of(group):
    first = max(3 * group // 8, 1)
    return [(0, first), (first, group - first)] if group > first else [(0, group)]


def encode(values, code_ref, step_ref, first=0):
    lane = lax.broadcasted_iota(jnp.int32, (1, 128), 1)
    steps = jnp.zeros((1, 128), jnp.float32)
    for i, value in enumerate(values):
        peak = jnp.max(jnp.max(jnp.abs(value), axis=0, keepdims=True), axis=1, keepdims=True)
        peak = jnp.maximum(peak, TINY)
        steps = jnp.where(lane == i, peak * (1.0 / LEVELS), steps)
        code = jnp.round(value * (LEVELS / peak)).astype(jnp.int32).astype(jnp.int16)
        code_ref[:, first + i] = code.reshape(-1, 2, value.shape[1])
    step_ref[...] = steps


def decode(code):
    rows = code.astype(jnp.int32).astype(jnp.float32)
    return rows.reshape(2 * code.shape[0], code.shape[2])


def stream_kernel(
    index_hbm,
    bank_hbm,
    flag_hbm,
    vis_ref,
    out_ref,
    index_ref,
    bank_ref,
    flag_ref,
    real_ref,
    imag_ref,
    good_ref,
    band_ref,
    slab_ref,
    sum_ref,
    edge_ref,
    edge_step_ref,
    mid_ref,
    mid_step_ref,
    in_ref,
    in_edge_step_ref,
    in_mid_step_ref,
    done_ref,
    own_ref,
    small_sem,
    load_sem,
    edge_send,
    edge_step_send,
    mid_send,
    mid_step_send,
    edge_recv,
    edge_step_recv,
    mid_recv,
    mid_step_recv,
    done_send,
    done_recv,
    own_sem,
    lefts_in,
    rights_in,
    *,
    count,
):
    me = lax.axis_index("tm")
    loads, block_rows, group, _, channels = slab_ref.shape
    chunks = done_ref.shape[0]
    per_owner = chunks // count
    out_count, edge, mid, edge_rows, mid_rows, total_rows, _ = row_plan(block_rows)
    alone = out_count - SIDE
    mid_at, far_at = edge_rows, edge_rows + mid_rows
    has_left, has_right = me > 0, me < count - 1
    nearer, farther = jnp.minimum(me, count - 1 - me), jnp.maximum(me, count - 1 - me)
    sign = jnp.where(2 * me <= count - 1, 1, -1)

    def chunk_at(step):
        turn, part = step // per_owner, step % per_owner
        late = turn - (farther - nearer)
        flip = jnp.where(late % 2 == 0, sign, -sign)
        owner = jnp.where(
            late < 0, me + sign * (farther - turn), me + flip * (nearer - late // 2)
        )
        return owner, part, owner * per_owner + part

    lots = lots_of(group)
    pieces = range(len(lots))

    def load(step, piece):
        _, _, chunk = chunk_at(step)
        slot = step % loads
        start, size = lots[piece]
        return pltpu.make_async_copy(
            vis_ref.at[:, pl.ds(chunk * group + start, size)],
            slab_ref.at[slot, :, pl.ds(start, size)],
            load_sem.at[slot, piece],
        )

    def remote(source, target, send_sem, recv_sem, device):
        return pltpu.make_async_remote_copy(
            src_ref=source,
            dst_ref=target,
            send_sem=send_sem,
            recv_sem=recv_sem,
            device_id={"tm": device},
            device_id_type=pl.DeviceIdType.MESH,
        )

    def slot_of(owner, part, chunk, receiver, rightward):
        second = jnp.logical_and(owner == receiver, jnp.logical_not(rightward))
        return jnp.where(second, chunks + part, chunk)

    def edge_copy(chunk, slot, rightward, device, piece):
        start = jnp.where(rightward, mid, 0)
        lot = pl.ds(*lots[piece])
        return remote(
            edge_ref.at[chunk, :, lot],
            in_ref.at[slot, pl.ds(start, edge), lot],
            edge_send.at[chunk, piece],
            edge_recv.at[slot, piece],
            device,
        )

    def edge_step_copy(chunk, slot, device):
        return remote(
            edge_step_ref.at[chunk],
            in_edge_step_ref.at[slot],
            edge_step_send.at[chunk],
            edge_step_recv.at[slot],
            device,
        )

    def edge_copies(chunk, slot, rightward, device):
        copies = [edge_copy(chunk, slot, rightward, device, piece) for piece in pieces]
        return copies + [edge_step_copy(chunk, slot, device)]

    def mid_copies(chunk, slot, rightward, device):
        start = jnp.where(rightward, 0, edge)
        return (
            remote(
                mid_ref.at[chunk],
                in_ref.at[slot, pl.ds(start, mid)],
                mid_send.at[chunk],
                mid_recv.at[slot],
                device,
            ),
            remote(
                mid_step_ref.at[chunk],
                in_mid_step_ref.at[slot],
                mid_step_send.at[chunk],
                mid_step_recv.at[slot],
                device,
            ),
        )

    def placed(row, rows, part):
        return out_ref.at[pl.ds(row, rows), pl.ds(part * group, group)]

    def full_done(source, chunk, part, rightward, device):
        row = jnp.where(rightward, out_count * (source - 1) + alone, out_count * source + SIDE)
        return remote(
            done_ref.at[chunk],
            placed(row, edge, part),
            done_send.at[chunk],
            done_recv.at[source, part],
            device,
        )

    def short_done(source, chunk, part, rightward, device):
        row = jnp.where(rightward, 0, out_count * source + SIDE)
        start = jnp.where(rightward, SIDE, 0)
        return remote(
            done_ref.at[chunk, pl.ds(start, alone)],
            placed(row, alone, part),
            done_send.at[chunk],
            done_recv.at[source, part],
            device,
        )

    def keep(part, low, rows):
        return pltpu.make_async_copy(
            own_ref.at[part, pl.ds(low, rows)],
            placed(jnp.maximum(out_count * me - SIDE, 0), rows, part),
            own_sem.at[part],
        )

    smalls = [
        pltpu.make_async_copy(source, target, small_sem.at[k])
        for k, (source, target) in enumerate(
            ((bank_hbm, bank_ref), (flag_hbm, flag_ref), (index_hbm, index_ref))
        )
    ]
    for copy in smalls:
        copy.start()
    for piece in pieces:
        load(0, piece).start()
    def signal(semaphore, device):
        pl.semaphore_signal(
            semaphore, inc=1, device_id={"tm": device}, device_id_type=pl.DeviceIdType.MESH
        )

    barrier = pltpu.get_barrier_semaphore()

    @pl.when(has_left)
    def _():
        signal(barrier, me - 1)

    @pl.when(has_right)
    def _():
        signal(barrier, me + 1)

    build_rows(bank_ref, flag_ref, real_ref, imag_ref, good_ref, block_rows, smalls)
    for step in range(1, loads - 1):
        for piece in pieces:
            load(step, piece).start()

    def flow(owner):
        rightward = owner > me
        upstream = jnp.where(rightward, has_left, has_right)
        return rightward, upstream, jnp.where(rightward, me + 1, me - 1)

    def baseline(chunk, slot, i, band):
        slab = slab_ref[slot, :, i].reshape(2 * block_rows, channels)
        both = jnp.dot(band, slab, preferred_element_type=jnp.float32)
        sum_ref[chunk, i] = both[:total_rows] + both[total_rows:]

    def rows_of(which):
        return real_ref[pl.ds(which, 1), :], imag_ref[pl.ds(which, 1), :]

    def send_edges(owner, part, chunk, piece):
        rightward, _, target = flow(owner)
        landing = slot_of(owner, part, chunk, target, rightward)
        near = pl.multiple_of(jnp.where(rightward, far_at, 0), 8)
        start, size = lots[piece]
        values = [
            sum_ref[chunk, i, pl.ds(near, 2 * edge), :] for i in range(start, start + size)
        ]
        encode(values, edge_ref.at[chunk], edge_step_ref.at[chunk, piece], start)
        edge_copy(chunk, landing, rightward, target, piece).start()
        if piece == len(lots) - 1:
            edge_step_copy(chunk, landing, target).start()

    def prefetch(step):
        @pl.when(step + loads - 1 < chunks)
        def _():
            for piece in pieces:
                load(step + loads - 1, piece).start()

    def compute_ends(step, carry):
        owner, part, chunk = chunk_at(step)
        _, upstream, _ = flow(owner)

        ends = jnp.logical_and(owner != me, jnp.logical_not(upstream))

        @pl.when(ends)
        def _():
            values = [sum_ref[chunk, i, mid_at : mid_at + 2 * mid, :] for i in range(group)]
            encode(values, mid_ref.at[chunk], mid_step_ref.at[chunk])

        turn = step // per_owner
        paired = jnp.logical_or(turn % 2 == 1, turn == count - 2)
        paired = jnp.logical_and(paired, part == per_owner - 1)

        @pl.when(jnp.logical_and(ends, paired))
        def _():
            def start_mid(back, carry):
                owner, part, chunk = chunk_at(back)
                rightward, _, target = flow(owner)
                landing = slot_of(owner, part, chunk, target, rightward)
                for copy in mid_copies(chunk, landing, rightward, target):
                    copy.start()
                return carry

            lax.fori_loop((turn - turn % 2) * per_owner, step + 1, start_mid, 0)

        return carry

    runs = runs_of(block_rows)

    def first_edges(run, near, rows):
        def one_chunk(step, carry):
            owner, part, chunk = chunk_at(step)
            for piece in pieces:
                load(step, piece).wait()
                for i in range(lots[piece][0], sum(lots[piece])):
                    real, imag = rows_of(index_ref[chunk * group + i])
                    band = build_band(real, imag, good_ref[...], block_rows, (run,))
                    slab = slab_ref[step % loads, :, i].reshape(2 * block_rows, channels)
                    both = jnp.dot(band, slab, preferred_element_type=jnp.float32)
                    sum_ref[chunk, i, near : near + rows, :] = both[:rows] + both[rows:]
                if piece == 0:

                    @pl.when(step == 0)
                    def _():
                        greeted = has_left.astype(jnp.int32) + has_right.astype(jnp.int32)
                        pl.semaphore_wait(barrier, greeted)

                send_edges(owner, part, chunk, piece)
            return carry

        lax.fori_loop(0, per_owner, one_chunk, 0)

    right_first = chunk_at(0)[0] > me

    @pl.when(right_first)
    def _():
        first_edges(runs[2], far_at, edge_rows)

    @pl.when(jnp.logical_not(right_first))
    def _():
        first_edges(runs[0], 0, edge_rows)

    def one_band(f, carry):
        band_ref[f] = build_band(*rows_of(f), good_ref[...], block_rows, runs)
        return carry

    lax.fori_loop(0, real_ref.shape[0], one_band, 0, unroll=2)

    def compute(step, carry):
        prefetch(step)
        owner, part, chunk = chunk_at(step)
        slot = step % loads

        @pl.when(step >= per_owner)
        def _():
            for piece in pieces:
                load(step, piece).wait()

        for i in range(group):
            baseline(chunk, slot, i, band_ref[index_ref[chunk * group + i]])

        @pl.when(jnp.logical_and(step >= per_owner, owner != me))
        def _():
            for piece in pieces:
                send_edges(owner, part, chunk, piece)

        return carry

    lax.fori_loop(0, chunks, lambda step, carry: compute_ends(step, compute(step, carry)), 0)

    @pl.when(has_left)
    def _():
        pl.semaphore_wait(lefts_in, 1)

    @pl.when(has_right)
    def _():
        signal(lefts_in, me + 1)
        pl.semaphore_wait(rights_in, 1)

    @pl.when(has_left)
    def _():
        signal(rights_in, me - 1)

    forward = chunks - per_owner

    def came(slot, start, rows, i):
        return decode(in_ref[slot, pl.ds(start, rows), i])

    def edge_unit(slot, i):
        piece = [i >= start for start, _ in lots].count(True) - 1
        lane = i - lots[piece][0]
        return in_edge_step_ref[slot, piece, :, lane : lane + 1]

    def pass_mid(step, carry):
        owner, part, chunk = chunk_at(step)
        rightward, upstream, target = flow(owner)
        landing = slot_of(owner, part, chunk, target, rightward)

        @pl.when(upstream)
        def _():
            for copy in edge_copies(chunk, chunk, rightward, target):
                copy.wait_recv()
            start = jnp.where(rightward, edge, 0)
            values = [
                sum_ref[chunk, i, mid_at : mid_at + 2 * mid, :]
                + came(chunk, start, mid, i) * edge_unit(chunk, i)
                for i in range(group)
            ]
            encode(values, mid_ref.at[chunk], mid_step_ref.at[chunk])
            for copy in mid_copies(chunk, landing, rightward, target):
                copy.start()

        return carry

    lax.fori_loop(0, forward, pass_mid, 0)

    def round_off(value, rows):
        return value.astype(jnp.bfloat16).reshape(rows, 2, channels)

    def pass_done(step, carry):
        owner, part, chunk = chunk_at(step)
        rightward, upstream, target = flow(owner)
        near = pl.multiple_of(jnp.where(rightward, 0, far_at), 8)

        @pl.when(upstream)
        def _():
            for copy in mid_copies(chunk, chunk, rightward, target):
                copy.wait_recv()
            start = jnp.where(rightward, 0, mid)
            at = lax.broadcasted_iota(jnp.int32, (2 * edge, channels), 0)
            first = jnp.where(rightward, 0, 2 * (edge - mid))
            of_mid = jnp.logical_and(at >= first, at < first + 2 * mid)
            mids = in_mid_step_ref[chunk]
            for i in range(group):
                unit = jnp.where(of_mid, mids[:, i : i + 1], edge_unit(chunk, i))
                value = sum_ref[chunk, i, pl.ds(near, 2 * edge), :]
                value = value + came(chunk, start, edge, i) * unit
                done_ref[chunk, :, i] = round_off(value, edge)
            full_done(me, chunk, part, rightward, owner).start()

        @pl.when(jnp.logical_not(upstream))
        def _():
            for i in range(group):
                value = sum_ref[chunk, i, pl.ds(near, 2 * edge), :]
                done_ref[chunk, :, i] = round_off(value, edge)
            short_done(me, chunk, part, rightward, owner).start()

        return carry

    lax.fori_loop(0, forward, pass_done, 0)

    def pass_own(part, carry):
        chunk = me * per_owner + part

        def from_side(slot, rightward, near, edge_start, first):
            for copy in edge_copies(chunk, slot, rightward, me):
                copy.wait_recv()
            for copy in mid_copies(chunk, slot, rightward, me):
                copy.wait_recv()
            at = lax.broadcasted_iota(jnp.int32, (2 * edge, channels), 0)
            of_mid = jnp.logical_and(at >= first, at < first + 2 * mid)
            mids = in_mid_step_ref[slot]
            start = edge if rightward else 0
            for i in range(group):
                unit = jnp.where(of_mid, mids[:, i : i + 1], edge_unit(slot, i))
                sum_ref[chunk, i, near : near + 2 * edge, :] += (
                    came(slot, edge_start, edge, i) * unit
                )
                sum_ref[chunk, i, mid_at : mid_at + 2 * mid, :] += (
                    came(slot, start, mid, i) * edge_unit(slot, i)
                )

        @pl.when(has_left)
        def _():
            from_side(chunk, True, 0, 0, 0)

        @pl.when(has_right)
        def _():
            from_side(chunks + part, False, far_at, mid, 2 * (edge - mid))

        for i in range(group):
            for row, rows, start in (
                (0, edge, 0),
                (edge, mid, mid_at),
                (edge + mid, edge, far_at),
            ):
                value = sum_ref[chunk, i, start : start + 2 * rows, :]
                own_ref[part, row : row + rows, i] = round_off(value, rows)

        @pl.when(jnp.logical_and(has_left, has_right))
        def _():
            keep(part, 0, 2 * edge + mid).start()

        @pl.when(jnp.logical_not(has_left))
        def _():
            keep(part, SIDE, out_count + SIDE).start()

        @pl.when(jnp.logical_not(has_right))
        def _():
            keep(part, 0, out_count + SIDE).start()

        return carry

    lax.fori_loop(0, per_owner, pass_own, 0)

    def drain(step, carry):
        owner, part, chunk = chunk_at(step)
        rightward, upstream, target = flow(owner)

        @pl.when(owner != me)
        def _():
            for copy in edge_copies(chunk, chunk, rightward, target):
                copy.wait_send()
            for copy in mid_copies(chunk, chunk, rightward, target):
                copy.wait_send()

            @pl.when(upstream)
            def _():
                full_done(me, chunk, part, rightward, owner).wait_send()

            @pl.when(jnp.logical_not(upstream))
            def _():
                short_done(me, chunk, part, rightward, owner).wait_send()

        @pl.when(owner == me)
        def _():
            @pl.when(jnp.logical_and(has_left, has_right))
            def _():
                keep(part, 0, 2 * edge + mid).wait()

            @pl.when(jnp.logical_not(jnp.logical_and(has_left, has_right)))
            def _():
                keep(part, 0, out_count + SIDE).wait()

        return carry

    lax.fori_loop(0, chunks, drain, 0)

    def collect(turn, carry):
        source = lax.rem(me + 1 + turn, count)
        end = jnp.logical_or(source == 0, source == count - 1)
        for part in range(per_owner):

            @pl.when(end)
            def _():
                short_done(source, 0, part, source < me, source).wait_recv()

            @pl.when(jnp.logical_not(end))
            def _():
                full_done(source, 0, part, source < me, source).wait_recv()

        return carry

    lax.fori_loop(0, count - 1, collect, 0)


def stream_call(kernel_index, filter_bank, flags, visibilities):
    block_rows, bases, _, channels = visibilities.shape
    count = lax.axis_size("tm")
    out_count, edge, mid, _, _, total_rows, period = row_plan(block_rows)
    filters = filter_bank.shape[1]
    owned = bases // count
    group = GROUP
    while owned % group:
        group //= 2
    chunks, parts, pieces = bases // group, owned // group, len(lots_of(group))
    slots = chunks + parts
    loads = max(LOADS, parts + 1)
    small = [
        pltpu.with_memory_space_constraint(operand, pltpu.HBM)
        for operand in (kernel_index, filter_bank, flags)
    ]
    sent, landed = pltpu.SemaphoreType.DMA((chunks,)), pltpu.SemaphoreType.DMA((slots,))
    return pl.pallas_call(
        functools.partial(stream_kernel, count=count),
        in_specs=[
            pl.BlockSpec(memory_space=pltpu.HBM),
            pl.BlockSpec(memory_space=pltpu.HBM),
            pl.BlockSpec(memory_space=pltpu.HBM),
            pl.BlockSpec(memory_space=pl.ANY),
        ],
        out_specs=pl.BlockSpec(memory_space=pl.ANY),
        out_shape=jax.ShapeDtypeStruct((count * out_count, owned, 2, channels), jnp.bfloat16),
        scratch_shapes=[
            pltpu.SMEM(kernel_index.shape, jnp.int32),
            pltpu.VMEM(filter_bank.shape, jnp.float32),
            pltpu.VMEM(flags.shape, jnp.int32),
            pltpu.VMEM((filters, period), jnp.float32),
            pltpu.VMEM((filters, period), jnp.float32),
            pltpu.VMEM((8, 2 * block_rows), jnp.float32),
            pltpu.VMEM((filters, 2 * total_rows, 2 * block_rows), jnp.bfloat16),
            pltpu.VMEM((loads, block_rows, group, 2, channels), jnp.bfloat16),
            pltpu.VMEM((chunks, group, total_rows, channels), jnp.float32),
            pltpu.VMEM((chunks, edge, group, 2, channels), jnp.int16),
            pltpu.VMEM((chunks, pieces, 1, 128), jnp.float32),
            pltpu.VMEM((chunks, mid, group, 2, channels), jnp.int16),
            pltpu.VMEM((chunks, 1, 128), jnp.float32),
            pltpu.VMEM((slots, edge + mid, group, 2, channels), jnp.int16),
            pltpu.VMEM((slots, pieces, 1, 128), jnp.float32),
            pltpu.VMEM((slots, 1, 128), jnp.float32),
            pltpu.VMEM((chunks, edge, group, 2, channels), jnp.bfloat16),
            pltpu.VMEM((parts, 2 * edge + mid, group, 2, channels), jnp.bfloat16),
            pltpu.SemaphoreType.DMA((3,)),
            pltpu.SemaphoreType.DMA((loads, pieces)),
            pltpu.SemaphoreType.DMA((chunks, pieces)),
            sent,
            sent,
            sent,
            pltpu.SemaphoreType.DMA((slots, pieces)),
            landed,
            landed,
            landed,
            sent,
            pltpu.SemaphoreType.DMA((count, parts)),
            pltpu.SemaphoreType.DMA((parts,)),
            pltpu.SemaphoreType.REGULAR,
            pltpu.SemaphoreType.REGULAR,
        ],
        compiler_params=pltpu.CompilerParams(
            collective_id=0, has_side_effects=True, vmem_limit_bytes=40 * 1024 * 1024
        ),
    )(*small, visibilities)


def per_device(visibilities, flag_mask, kernel_index, filter_bank):
    return stream_call(kernel_index, filter_bank, flag_mask[None, :], visibilities)


def solution(mesh):
    placed = (
        P(("group", "tm"), ("bl", "pol"), None, None),
        P(("group", "tm")),
        P(("bl", "pol")),
        P(),
    )
    return jax.shard_map(
        per_device,
        mesh=mesh,
        in_specs=placed,
        out_specs=P("group", ("bl", "pol", "tm"), None, None),
        check_vma=False,
    )
```
